128 devices in a mesh: gx: 2 (over core), gy: 32 (over z, y, x_hi), gz: 2 (over x_lo).
Axes of the slice: x: 4 (x_hi: 2, x_lo: 2; x = x_hi * 2 + x_lo), y: 4, z: 4, core: 2. Of those that a mesh axis runs over, the one named last changes fastest.
Arguments:
- number_densities: float32 [64, 8, 128, 256], P(None, 'gx', 'gy', 'gz'), may hold values from 0.0125 to 24, as said below
- kinetic_kelvin: float32 [8, 128, 256], P('gx', 'gy', 'gz'), may hold values from 0.5 to 3
- flow_vector: float32 [3, 8, 128, 256], P(None, 'gx', 'gy', 'gz'), may hold values from -1 to 1
- opacity_area: float32 [128, 64], replicated, may hold values from 0.0078125 to 0.078125
- illumination: float32 [6], replicated, may hold values from 0.2 to 1
- arrhenius_coefficient: float32 [128], replicated, may hold values from 0.1 to 1
- arrhenius_barrier: float32 [128], replicated, may hold values from 0.5 to 5
- exothermic_energy: float32 [256], replicated, may hold values from 0.002 to 0.02
- emission_loss: float32 [64], replicated, may hold values from 0.01 to 0.1
- participant_indices: int32 [4, 256], replicated, may hold values from 0 to 63
- demanding_patches: int32 [2, 32, 2, 4], P('gx', 'gy', 'gz'), may hold values from 0 to 16, as said below
Outputs:
- ending_populations: float32 [64, 8, 128, 256], P(None, 'gx', 'gy', 'gz')
- ending_warmth: float32 [8, 128, 256], P('gx', 'gy', 'gz')
The draws below stay inside these ranges and needn't reach their ends.
Inputs may be any that keep to these rules, and one draw needn't show every extreme that they name: `participant_indices`: stoichiometry names species. `number_densities`: densities are positive. `demanding_patches`: each brick's row holds distinct tile numbers first and 16 in its remaining slots; a brick lists at most 4 tiles and some brick lists exactly 4; the 2 bricks that share their first two brick indices together list exactly 4 tiles.
All inputs are finite; a program needn't handle non-finite values.
Results may differ from the reference program's by a relative error of at most 0.0003.
Values sent between devices are 32-bit elements; how exact they have to be, the bound alone decides.
No kernel may reach another device: no remote copies, remote signals or barrier semaphores. Data moves between devices by JAX's collectives and lax.ppermute only.
A program may use at most 64 MiB of HBM per device.

```python
import math
from functools import partial
import jax
import jax.numpy as jnp
from jax import lax

KINDS = 64
R = 256
PHOTON_COUNT = 128
TWO = 128
NSUB = 8
BLOCK_SPAN_EAST = 4
BLOCK_SPAN_NORTH = 4
BLOCK_SPAN_UPWARD = 128
BX = 2
BY = 32
BZ = 2
MESH_SPAN_EAST = 8
MESH_SPAN_NORTH = 128
MESH_SPAN_UPWARD = 256
PATCH_COUNT = 16
MAXD = 4
N_GX = 2
N_GY = 32
N_GZ = 2


def draw_number_densities(key, part):
    base = jax.random.fold_in(key, 29)
    cell_key, line_key = jax.random.split(base, 2)
    cell_log = jax.random.uniform(cell_key, (KINDS, MESH_SPAN_EAST, MESH_SPAN_NORTH, MESH_SPAN_UPWARD), jnp.float32, jnp.log(0.1), jnp.log(3.0))
    line_log = jax.random.uniform(line_key, (KINDS, 1, MESH_SPAN_NORTH, 1), jnp.float32, jnp.log(0.125), jnp.log(8.0))
    return jnp.exp(cell_log + line_log).astype(jnp.float32)


def draw_demanding_patches(key, part):
    line_count = BX * BY
    base = jax.random.fold_in(key, 17)
    ordering_key, share_key, tile_key = jax.random.split(base, 3)
    ordering = jax.vmap(lambda sub: jax.random.permutation(sub, BZ))(jax.random.split(ordering_key, line_count))
    shares = jax.random.randint(share_key, (line_count, BZ // 2), 0, MAXD + 1)
    shares = shares.at[0, 0].set(0)
    paired = jnp.stack([MAXD - shares, shares], axis=-1).reshape(line_count, BZ)
    line_index = jnp.arange(line_count)[:, None]
    counts = jnp.zeros((line_count, BZ), jnp.int32).at[line_index, ordering].set(paired.astype(jnp.int32))
    chosen_tiles = jax.vmap(lambda sub: jax.random.permutation(sub, PATCH_COUNT)[:MAXD])(jax.random.split(tile_key, line_count * BZ))
    slot_index = jnp.arange(MAXD)[None, :]
    enumerated = jnp.where(slot_index < counts.reshape(-1, 1), chosen_tiles, PATCH_COUNT)
    return enumerated.reshape(BX, BY, BZ, MAXD).astype(jnp.int32)


def with_ends(entries, stream_key, low, high):
    index_at = [jax.random.randint(jax.random.fold_in(stream_key, axis), (), 0, length) for axis, length in enumerate(entries.shape)]
    widest = entries.shape.index(max(entries.shape))
    beside = index_at[:widest] + [(index_at[widest] + 1) % entries.shape[widest]] + index_at[widest + 1:]
    return entries.at[tuple(index_at)].set(low).at[tuple(beside)].set(high)


def shard_levels(stream_key, shape, cuts, least, high):
    loudness, own = 1.0, jax.random.fold_in(stream_key, 6)
    for position, parts in cuts:
        draws = jnp.exp(jax.random.uniform(jax.random.fold_in(own, position), (parts,), jnp.float32, least / len(cuts), high / len(cuts)))
        loudness = loudness * jnp.repeat(draws, shape[position] // parts).reshape([-1 if axis == position else 1 for axis in range(len(shape))])
    return loudness


def setup_inputs(seed: int = 0) -> dict:
    keys = jax.random.split(jax.random.key(seed), 12)
    return {
        "number_densities": draw_number_densities(jax.random.fold_in(keys[11], 71), 0),
        "kinetic_kelvin": jnp.clip(jnp.exp(math.log(3.0) - 1.7917595 * jax.random.uniform(keys[1], (MESH_SPAN_EAST, MESH_SPAN_NORTH, MESH_SPAN_UPWARD), jnp.float32) ** shard_levels(keys[1], (MESH_SPAN_EAST, MESH_SPAN_NORTH, MESH_SPAN_UPWARD), ((0, 2), (1, 32), (2, 2)), -0.2, 0.2)), 0.5, 3.0),
        "flow_vector": jnp.clip(jax.random.uniform(keys[2], (3, MESH_SPAN_EAST, MESH_SPAN_NORTH, MESH_SPAN_UPWARD), jnp.float32, -1.0, 1.0) * shard_levels(keys[2], (3, MESH_SPAN_EAST, MESH_SPAN_NORTH, MESH_SPAN_UPWARD), ((1, 2), (2, 32), (3, 2)), -0.4, 0.0), -1.0, 1.0),
        "opacity_area": jnp.clip(jnp.exp(jax.random.uniform(keys[3], (PHOTON_COUNT, KINDS), jnp.float32, math.log(0.0078125), math.log(0.078125))), 0.0078125, 0.078125),
        "illumination": jnp.clip(jnp.exp(jax.random.uniform(keys[4], (6,), jnp.float32, math.log(0.2), math.log(1.0))), 0.2, 1.0),
        "arrhenius_coefficient": jnp.clip(jnp.exp(jax.random.uniform(keys[5], (TWO,), jnp.float32, math.log(0.1), math.log(1.0))), 0.1, 1.0),
        "arrhenius_barrier": jnp.clip(jnp.exp(jax.random.uniform(keys[6], (TWO,), jnp.float32, math.log(0.5), math.log(5.0))), 0.5, 5.0),
        "exothermic_energy": jnp.clip(jnp.exp(jax.random.uniform(keys[7], (R,), jnp.float32, math.log(0.002), math.log(0.02))), 0.002, 0.02),
        "emission_loss": jnp.clip(jnp.exp(jax.random.uniform(keys[8], (KINDS,), jnp.float32, math.log(0.01), math.log(0.1))), 0.01, 0.1),
        "participant_indices": with_ends(jax.random.randint(keys[9], (4, R), 0, KINDS), jax.random.fold_in(keys[9], 1), 0, KINDS - 1).astype(jnp.int32),
        "demanding_patches": draw_demanding_patches(jax.random.fold_in(keys[11], 71), 0),
    }


HIGHEST = lax.Precision.HIGHEST
whole_update = 1.0
courant = 0.25


def reaction_tables(participant_indices):
    species = jnp.arange(KINDS, dtype=jnp.int32)[:, None]
    onehot_first = (participant_indices[0][None, :] == species).astype(jnp.float32)
    onehot_second = (participant_indices[1][None, :] == species).astype(jnp.float32)
    produced = (participant_indices[2][None, :] == species).astype(jnp.float32) + (participant_indices[3][None, :] == species).astype(jnp.float32)
    losing = jnp.concatenate([onehot_first, onehot_second[:, PHOTON_COUNT:]], axis=1)
    return produced, losing


def kinetics_advance(particle_count, voxel_warmth, photolysis_speed, lookup_arrays, participant_indices, arrhenius_coefficient, arrhenius_barrier, exothermic_energy, emission_loss, timestep_length):
    produced, losing = lookup_arrays
    reactant = jnp.take(particle_count, participant_indices[0], axis=0)
    partner = jnp.take(particle_count, participant_indices[1, PHOTON_COUNT:], axis=0)
    energetic_update = arrhenius_coefficient[:, None] * jnp.exp(-arrhenius_barrier[:, None] / voxel_warmth[None, :])
    reaction = jnp.concatenate([photolysis_speed * reactant[:PHOTON_COUNT], energetic_update * reactant[PHOTON_COUNT:] * partner], axis=0)
    removal = jnp.concatenate([photolysis_speed, energetic_update * partner, energetic_update * reactant[PHOTON_COUNT:]], axis=0)
    gained = jnp.dot(produced, reaction, precision=HIGHEST)
    loss_sum = jnp.dot(losing, removal, precision=HIGHEST)
    energy_gain = jnp.dot(exothermic_energy, reaction, precision=HIGHEST)
    energy_drain = jnp.dot(emission_loss, particle_count, precision=HIGHEST)
    new_density = (particle_count + timestep_length * gained) / (1.0 + timestep_length * loss_sum)
    updated_kelvin = (voxel_warmth + timestep_length * energy_gain) / (1.0 + timestep_length * energy_drain)
    return new_density, updated_kelvin


def advance(packed, kinetics_scheme, inner_increments):
    tile_count = packed.shape[1]
    voxels = packed.shape[2]
    cohort = math.gcd(tile_count, 16)
    grouped = packed.reshape(packed.shape[0], tile_count // cohort, cohort, voxels).transpose(1, 0, 2, 3)

    def one_group(fragment):
        particle_count = fragment[:KINDS].reshape(KINDS, -1)
        voxel_warmth = fragment[KINDS].reshape(-1)
        photolysis_speed = fragment[KINDS + 1:].reshape(PHOTON_COUNT, -1)
        for substep in range(inner_increments):
            particle_count, voxel_warmth = kinetics_advance(particle_count, voxel_warmth, photolysis_speed, *kinetics_scheme, whole_update / inner_increments)
        return particle_count.reshape(KINDS, cohort, voxels), voxel_warmth.reshape(cohort, voxels)

    group_density, group_warmth = lax.map(one_group, grouped)
    return group_density.transpose(1, 0, 2, 3).reshape(KINDS, tile_count, voxels), group_warmth.reshape(tile_count, voxels)


def line_columns(particle_count, beneath, overhead, along):
    running = jnp.cumsum(particle_count, axis=along)
    line_total = jnp.sum(particle_count, axis=along, keepdims=True)
    lower_part = beneath + (running - particle_count) + 0.5 * particle_count
    upper_part = overhead + (line_total - running) + 0.5 * particle_count
    return lower_part, upper_part


def photo_rates(columns, opacity_area, illumination, block_extents):
    summed = None
    for direction in range(6):
        optical = jnp.dot(opacity_area, columns[direction].reshape(KINDS, -1), precision=HIGHEST) / block_extents[direction // 2]
        shielded = illumination[direction] * jnp.exp(-optical)
        summed = shielded if direction == 0 else summed + shielded
    return summed


def block_contents(particle_count, voxel_warmth, block_bounds, block_extents, opacity_area, illumination, kinetics_scheme):
    columns = []
    for along in range(3):
        beneath, overhead = block_bounds[along]
        columns.extend(line_columns(particle_count, beneath, overhead, along + 1))
    photolysis_speed = photo_rates(columns, opacity_area, illumination, block_extents)
    piled_together = jnp.concatenate([particle_count.reshape(KINDS, PATCH_COUNT, -1), voxel_warmth.reshape(1, PATCH_COUNT, -1), photolysis_speed.reshape(PHOTON_COUNT, PATCH_COUNT, -1)], axis=0)
    calm_populations, calm_kelvin = advance(piled_together, kinetics_scheme, 1)
    return calm_populations, calm_kelvin, piled_together


def insert_tiles(calm_populations, calm_kelvin, enumerated, tile_density, patch_kelvin):
    particle_count = calm_populations.at[:, enumerated].set(tile_density, mode="drop")
    voxel_warmth = calm_kelvin.at[enumerated].set(patch_kelvin, mode="drop")
    return particle_count.reshape(KINDS, BLOCK_SPAN_EAST, BLOCK_SPAN_NORTH, -1), voxel_warmth.reshape(BLOCK_SPAN_EAST, BLOCK_SPAN_NORTH, -1)


def brick_offsets(number_densities, along, blocks, width):
    full_shape = number_densities.shape
    split_shape = full_shape[:along] + (blocks, width) + full_shape[along + 1:]
    totals = jnp.sum(number_densities.reshape(split_shape), axis=along + 1)
    running = jnp.cumsum(totals, axis=along)
    return running - totals, jnp.sum(totals, axis=along, keepdims=True) - running


def block_starts(*values):
    return tuple(jnp.asarray(value, jnp.int32) for value in values)


def advect_field(values, flow_vector):
    change = None
    for along in range(3):
        speed_along = flow_vector[along]
        face_speed = 0.5 * (speed_along + jnp.roll(speed_along, -1, along))
        face_flux = jnp.where(face_speed > 0,
                              face_speed * (1.5 * values - 0.5 * jnp.roll(values, 1, along)),
                              face_speed * (1.5 * jnp.roll(values, -1, along) - 0.5 * jnp.roll(values, -2, along)))
        difference = face_flux - jnp.roll(face_flux, 1, along)
        change = difference if along == 0 else change + difference
    return values - courant * change


def reference(number_densities, kinetic_kelvin, flow_vector, opacity_area, illumination, arrhenius_coefficient, arrhenius_barrier, exothermic_energy, emission_loss, participant_indices, demanding_patches):
    kinetics_scheme = (reaction_tables(participant_indices), participant_indices, arrhenius_coefficient, arrhenius_barrier, exothermic_energy, emission_loss)
    offsets_x = brick_offsets(number_densities, 1, N_GX, BLOCK_SPAN_EAST)
    offsets_y = brick_offsets(number_densities, 2, N_GY, BLOCK_SPAN_NORTH)
    offsets_z = brick_offsets(number_densities, 3, N_GZ, BLOCK_SPAN_UPWARD)
    block_extents = (float(MESH_SPAN_EAST), float(MESH_SPAN_NORTH), float(MESH_SPAN_UPWARD))
    listing = demanding_patches.reshape(-1, MAXD)
    zero = jnp.asarray(0, jnp.int32)

    def single_block(number):
        block_eastward = number // (N_GY * N_GZ)
        block_northward = (number // N_GZ) % N_GY
        block_upward = number % N_GZ
        particle_count = lax.dynamic_slice(number_densities, block_starts(zero, block_eastward * BLOCK_SPAN_EAST, block_northward * BLOCK_SPAN_NORTH, block_upward * BLOCK_SPAN_UPWARD), (KINDS, BLOCK_SPAN_EAST, BLOCK_SPAN_NORTH, BLOCK_SPAN_UPWARD))
        voxel_warmth = lax.dynamic_slice(kinetic_kelvin, block_starts(block_eastward * BLOCK_SPAN_EAST, block_northward * BLOCK_SPAN_NORTH, block_upward * BLOCK_SPAN_UPWARD), (BLOCK_SPAN_EAST, BLOCK_SPAN_NORTH, BLOCK_SPAN_UPWARD))
        start_x = block_starts(zero, block_eastward, block_northward * BLOCK_SPAN_NORTH, block_upward * BLOCK_SPAN_UPWARD)
        start_y = block_starts(zero, block_eastward * BLOCK_SPAN_EAST, block_northward, block_upward * BLOCK_SPAN_UPWARD)
        start_z = block_starts(zero, block_eastward * BLOCK_SPAN_EAST, block_northward * BLOCK_SPAN_NORTH, block_upward)
        block_bounds = (
            (lax.dynamic_slice(offsets_x[0], start_x, (KINDS, 1, BLOCK_SPAN_NORTH, BLOCK_SPAN_UPWARD)), lax.dynamic_slice(offsets_x[1], start_x, (KINDS, 1, BLOCK_SPAN_NORTH, BLOCK_SPAN_UPWARD))),
            (lax.dynamic_slice(offsets_y[0], start_y, (KINDS, BLOCK_SPAN_EAST, 1, BLOCK_SPAN_UPWARD)), lax.dynamic_slice(offsets_y[1], start_y, (KINDS, BLOCK_SPAN_EAST, 1, BLOCK_SPAN_UPWARD))),
            (lax.dynamic_slice(offsets_z[0], start_z, (KINDS, BLOCK_SPAN_EAST, BLOCK_SPAN_NORTH, 1)), lax.dynamic_slice(offsets_z[1], start_z, (KINDS, BLOCK_SPAN_EAST, BLOCK_SPAN_NORTH, 1))),
        )
        calm_populations, calm_kelvin, piled_together = block_contents(particle_count, voxel_warmth, block_bounds, block_extents, opacity_area, illumination, kinetics_scheme)
        enumerated = listing[number]
        chosen = jnp.minimum(enumerated, PATCH_COUNT - 1)
        packed = jnp.take(piled_together, chosen, axis=1)
        tile_density, patch_kelvin = advance(packed, kinetics_scheme, NSUB)
        return insert_tiles(calm_populations, calm_kelvin, enumerated, tile_density, patch_kelvin)

    block_numbers, block_warmth = lax.map(single_block, jnp.arange(N_GX * N_GY * N_GZ, dtype=jnp.int32))
    chem_abundance = block_numbers.reshape(N_GX, N_GY, N_GZ, KINDS, BLOCK_SPAN_EAST, BLOCK_SPAN_NORTH, BLOCK_SPAN_UPWARD).transpose(3, 0, 4, 1, 5, 2, 6).reshape(KINDS, MESH_SPAN_EAST, MESH_SPAN_NORTH, MESH_SPAN_UPWARD)
    ending_warmth = block_warmth.reshape(N_GX, N_GY, N_GZ, BLOCK_SPAN_EAST, BLOCK_SPAN_NORTH, BLOCK_SPAN_UPWARD).transpose(0, 3, 1, 4, 2, 5).reshape(MESH_SPAN_EAST, MESH_SPAN_NORTH, MESH_SPAN_UPWARD)
    ending_populations = lax.map(partial(advect_field, flow_vector=flow_vector), chem_abundance)
    return ending_populations, ending_warmth
```

```python
import functools

import jax
import jax.numpy as jnp
from jax import lax
from jax.experimental import pallas as pl
from jax.experimental.pallas import tpu as pltpu
from jax.sharding import PartitionSpec as P

KINDS = 64
PHOTON = 128
NSUB = 8
TILES = 16
LANES = 128
MAXD = 4
LOG2E = 1.4426950408889634

F32 = jnp.float32
BF16 = jnp.bfloat16


def split(x):
    hi = x.astype(BF16)
    lo = (x - hi.astype(F32)).astype(BF16)
    return hi, lo


def dot(a, b):
    return jnp.dot(a, b, preferred_element_type=F32)


def totals_kernel(n_ref, v_ref, n2_ref, ty_ref, xpay_ref, zpay_ref):
    tiles = []
    for t in range(TILES):
        a = n_ref[pl.ds(t, KINDS, stride=TILES), :]
        n2_ref[t] = a
        tiles.append(a)
    for q in range(4):
        ty_ref[pl.ds(q * KINDS, KINDS), :] = (tiles[4 * q] + tiles[4 * q + 1]) + (
            tiles[4 * q + 2] + tiles[4 * q + 3]
        )
        xpay_ref[pl.ds(q * KINDS, KINDS), :] = (tiles[q] + tiles[q + 4]) + (
            tiles[q + 8] + tiles[q + 12]
        )
    lane = lax.broadcasted_iota(jnp.int32, (KINDS, LANES), 1)
    tz = jnp.zeros((KINDS, LANES), F32)
    for t in range(TILES):
        tz = jnp.where(lane == t, jnp.sum(tiles[t], axis=1, keepdims=True), tz)
    zpay_ref[pl.ds(0, KINDS), :] = tz
    xpay_ref[pl.ds(256, TILES), :] = v_ref[pl.ds(0, TILES), :]
    zpay_ref[pl.ds(KINDS, TILES), :] = v_ref[pl.ds(2 * TILES, TILES), :]


def chem(n, temp, photo, thermal, loss_light, g2, pg, lt, emission, h):
    hi, lo = split(n)
    gat = dot(g2, jnp.concatenate([hi, lo], axis=0))
    na, nb = gat[128:256], gat[256:384]
    kb = thermal * nb
    ka = thermal * na
    rate = jnp.concatenate([photo * gat[:128], kb * na], axis=0)
    rem = jnp.concatenate([kb, ka], axis=0)
    made = dot(pg, jnp.concatenate(split(rate), axis=0))
    lost = dot(lt, jnp.concatenate(split(rem), axis=0)) + loss_light
    heat = made[64:65] + made[65:66]
    cool = jnp.sum(emission * n, axis=0, keepdims=True)
    new_n = (n + h * made[:64]) / (1.0 + h * lost)
    new_t = (temp + h * heat) / (1.0 + h * cool)
    return new_n, new_t


def thermal_rates(temp, coef, barrier):
    return coef * jnp.exp2(barrier * (1.0 / temp))


def wide(parts):
    return jnp.concatenate(parts, axis=1)


def chemistry_kernel(
    where_ref, light_ref, listed_ref,
    n2_ref, temp_ref, v_ref, xown_ref, xpay_ref, yb_ref, yt_ref, zown_ref, zpay_ref,
    ost_ref, uu_ref, g2_ref, pg_ref, lt_ref, lp_ref, cols_ref, em_ref,
    n_out, temp_out, up_out, dn_out, z_out,
    cz_ref, ph_ref, ll_ref, cur_ref, curt_ref,
):
    gx, gz = where_ref[0], where_ref[1]
    for c in range(4):
        blk = n2_ref[pl.ds(c * 4, 4)].reshape(256, LANES)
        cz_ref[pl.ds(c * 256, 256), :] = dot(wide(split(blk)), uu_ref[...])
    ost = ost_ref[...]
    zsum = zown_ref[pl.ds(0, KINDS), :] + zpay_ref[pl.ds(0, KINDS), :]
    zlow = gz * zpay_ref[pl.ds(0, KINDS), :]
    runx = [gx * xpay_ref[pl.ds(q * KINDS, KINDS), :] for q in range(4)]
    for i in range(4):
        runy = yb_ref[pl.ds(i * KINDS, KINDS), :]
        ysum = yt_ref[pl.ds(i * KINDS, KINDS), :]
        for j in range(4):
            t = i * 4 + j
            n = n2_ref[t]
            half = 0.5 * n
            xl = runx[j] + half
            runx[j] = runx[j] + n
            yl = runy + half
            runy = runy + n
            zl = cz_ref[pl.ds(t * KINDS, KINDS), :] + zlow[:, t : t + 1]
            xsum = xown_ref[pl.ds(j * KINDS, KINDS), :] + xpay_ref[pl.ds(j * KINDS, KINDS), :]
            six = wide([xl, xsum - xl, yl, ysum - yl, zl, zsum[:, t : t + 1] - zl])
            hi, lo = split(six)
            tau = dot(ost, jnp.concatenate([hi, lo, hi], axis=0))
            ph = None
            for d in range(6):
                size = (8.0, 128.0, 256.0)[d // 2]
                part = light_ref[d] * jnp.exp2(tau[:, d * 128 : (d + 1) * 128] * (-LOG2E / size))
                ph = part if d == 0 else ph + part
            ph_ref[t] = ph

    g2, pg, lt, lp = g2_ref[...], pg_ref[...], lt_ref[...], lp_ref[...]
    coef = cols_ref[:, 0:1]
    barrier = cols_ref[:, 1:2]
    em = em_ref[:, 0:1]

    def quiet(c, carry):
        base = c * 4
        for p in range(2):
            a = base + 2 * p
            n = wide([n2_ref[a], n2_ref[a + 1]])
            temp = wide([temp_ref[pl.ds(a, 1), :], temp_ref[pl.ds(a + 1, 1), :]])
            ph = wide([ph_ref[a], ph_ref[a + 1]])
            ll = dot(lp, jnp.concatenate(split(ph), axis=0))
            ll_ref[a] = ll[:, :LANES]
            ll_ref[a + 1] = ll[:, LANES:]
            th = thermal_rates(temp, coef, barrier)
            nn, tt = chem(n, temp, ph, th, ll, g2, pg, lt, em, 1.0)
            n_out[a] = nn[:, :LANES]
            n_out[a + 1] = nn[:, LANES:]
            temp_out[pl.ds(a, 1), :] = tt[:, :LANES]
            temp_out[pl.ds(a + 1, 1), :] = tt[:, LANES:]
        return carry

    lax.fori_loop(0, 4, quiet, 0)

    pick = [jnp.minimum(listed_ref[m], TILES - 1) for m in range(MAXD)]
    for m in range(MAXD):
        cur_ref[m] = n2_ref[pick[m]]
        curt_ref[pl.ds(m, 1), :] = temp_ref[pl.ds(pick[m], 1), :]

    def substep(s, carry):
        for p in range(2):
            a, b = 2 * p, 2 * p + 1
            n = wide([cur_ref[a], cur_ref[b]])
            temp = wide([curt_ref[a : a + 1, :], curt_ref[b : b + 1, :]])
            ph = wide([ph_ref[pick[a]], ph_ref[pick[b]]])
            ll = wide([ll_ref[pick[a]], ll_ref[pick[b]]])
            th = thermal_rates(temp, coef, barrier)
            nn, tt = chem(n, temp, ph, th, ll, g2, pg, lt, em, 1.0 / NSUB)
            cur_ref[a] = nn[:, :LANES]
            cur_ref[b] = nn[:, LANES:]
            curt_ref[a : a + 1, :] = tt[:, :LANES]
            curt_ref[b : b + 1, :] = tt[:, LANES:]
        return carry

    lax.fori_loop(0, NSUB, substep, 0)

    for m in range(MAXD):

        @pl.when(listed_ref[m] < TILES)
        def _():
            n_out[pick[m]] = cur_ref[m]
            temp_out[pl.ds(pick[m], 1), :] = curt_ref[m : m + 1, :]

    lane = lax.broadcasted_iota(jnp.int32, (KINDS, LANES), 1)
    zp = jnp.zeros((KINDS, LANES), F32)
    up_out[pl.ds(512, 8), :] = jnp.zeros((8, LANES), F32)
    dn_out[pl.ds(512, 8), :] = jnp.zeros((8, LANES), F32)
    for i in range(4):
        for j in range(4):
            t = i * 4 + j
            u = n_out[t]
            zp = jnp.where(lane // 4 == t, pltpu.roll(u, 4 * t + 2, 1), zp)
            if j < 2:
                dn_out[pl.ds((j * 4 + i) * KINDS, KINDS), :] = u
            else:
                up_out[pl.ds(((j - 2) * 4 + i) * KINDS, KINDS), :] = u
        up_out[pl.ds(512 + i, 1), :] = v_ref[pl.ds(TILES + i * 4 + 3, 1), :]
        dn_out[pl.ds(512 + i, 1), :] = v_ref[pl.ds(TILES + i * 4, 1), :]
    z_out[...] = zp


def transport_kernel(n_ref, v_ref, hx_ref, xpay_ref, lo_ref, hi_ref, hz_ref, zpay_ref, out_ref):
    lane = lax.broadcasted_iota(jnp.int32, (KINDS, LANES), 1)
    lane1 = lax.broadcasted_iota(jnp.int32, (1, LANES), 1)

    def flux(face, um1, u, up1, up2):
        state = jnp.where(face > 0, 1.5 * u - 0.5 * um1, 1.5 * up1 - 0.5 * up2)
        return face * state

    def x_u(i, j):
        if 0 <= i < 4:
            return n_ref[i * 4 + j]
        return hx_ref[(i % 4) * 4 + j]

    def x_v(i, j):
        if 0 <= i < 4:
            return v_ref[i * 4 + j : i * 4 + j + 1, :]
        r = 256 + (i % 4) * 4 + j
        return xpay_ref[r : r + 1, :]

    def y_u(i, j):
        if j < 0:
            return lo_ref[pl.ds(((j + 2) * 4 + i) * KINDS, KINDS), :]
        if j > 3:
            return hi_ref[pl.ds(((j - 4) * 4 + i) * KINDS, KINDS), :]
        return n_ref[i * 4 + j]

    def y_v(i, j):
        if j < 0:
            return lo_ref[512 + i : 513 + i, :]
        if j > 3:
            return hi_ref[512 + i : 513 + i, :]
        return v_ref[16 + i * 4 + j : 17 + i * 4 + j, :]

    def x_flux(i, j):
        face = 0.5 * (x_v(i, j) + x_v(i + 1, j))
        return flux(face, x_u(i - 1, j), x_u(i, j), x_u(i + 1, j), x_u(i + 2, j))

    def y_flux(i, j):
        face = 0.5 * (y_v(i, j) + y_v(i, j + 1))
        return flux(face, y_u(i, j - 1), y_u(i, j), y_u(i, j + 1), y_u(i, j + 2))

    hz = hz_ref[...]
    xf = [x_flux(-1, j) for j in range(4)]
    for i in range(4):
        yf = y_flux(i, -1)
        for j in range(4):
            t = i * 4 + j
            u = n_ref[t]
            top = x_flux(i, j)
            change = top - xf[j]
            xf[j] = top
            top = y_flux(i, j)
            change = change + (top - yf)
            yf = top
            r = pltpu.roll(hz, (LANES - (4 * t + 2)) % LANES, 1)
            vz = v_ref[32 + t : 33 + t, :]
            pz = zpay_ref[64 + t : 65 + t, :]
            vup = pltpu.roll(jnp.where(lane1 == 0, pz, vz), LANES - 1, 1)
            face = 0.5 * (vz + vup)
            facelow = 0.5 * (pz + pltpu.roll(vz, LANES - 1, 1))
            r1, l1, l2 = (
                pltpu.roll(u, 1, 1), pltpu.roll(u, LANES - 1, 1), pltpu.roll(u, LANES - 2, 1),
            )
            q1, p1, p2 = (
                pltpu.roll(r, 1, 1), pltpu.roll(r, LANES - 1, 1), pltpu.roll(r, LANES - 2, 1),
            )
            fz = flux(
                face,
                jnp.where(lane == 0, q1, r1),
                u,
                jnp.where(lane == LANES - 1, p1, l1),
                jnp.where(lane >= LANES - 2, p2, l2),
            )
            flow = flux(facelow, q1, r, l1, l2)
            below = pltpu.roll(jnp.where(lane == LANES - 1, flow, fz), 1, 1)
            change = change + (fz - below)
            out_ref[pl.ds(t, KINDS, stride=TILES), :] = u - 0.25 * change


def sds(*shape):
    return jax.ShapeDtypeStruct(shape, F32)


VM = pl.BlockSpec(memory_space=pltpu.VMEM)
SM = pl.BlockSpec(memory_space=pltpu.SMEM)


def shards(
    number_densities, kinetic_kelvin, flow_vector, opacity_area, illumination,
    arrhenius_coefficient, arrhenius_barrier, exothermic_energy, emission_loss,
    participant_indices, demanding_patches,
):
    n = number_densities.reshape(KINDS * TILES, LANES)
    v = flow_vector.reshape(3 * TILES, LANES)
    temp = kinetic_kelvin.reshape(TILES, LANES)
    n2, ty, xown, zown = pl.pallas_call(
        totals_kernel,
        out_shape=(sds(TILES, KINDS, LANES), sds(256, LANES), sds(272, LANES), sds(80, LANES)),
        in_specs=[VM, VM],
        out_specs=(VM, VM, VM, VM),
        name="totals",
    )(n, v)

    gx, gy, gz = lax.axis_index("gx"), lax.axis_index("gy"), lax.axis_index("gz")
    size = lax.axis_size("gy")
    gx_size, gz_size = lax.axis_size("gx"), lax.axis_size("gz")
    around = lambda count, by: [(a, (a + by) % count) for a in range(count)]

    first = lax.ppermute(ty, "gy", [(a, a ^ 1) for a in range(size)])
    xpay = lax.ppermute(xown, "gx", around(gx_size, 1))
    zpay = lax.ppermute(zown, "gz", around(gz_size, 1))
    beneath = jnp.where(gy % 2 == 1, first, 0.0)
    total = ty + first
    row = (gy // 2) % 4
    got = [
        lax.ppermute(
            total, "gy", [(a, (a // 8) * 8 + ((a // 2 + k) % 4) * 2 + a % 2) for a in range(size)]
        )
        for k in (1, 2, 3)
    ]
    for k in (1, 2, 3):
        beneath = beneath + jnp.where(row >= k, got[k - 1], 0.0)
        total = total + got[k - 1]
    plane = gy // 8
    got = [lax.ppermute(total, "gy", around(size, 8 * k)) for k in (1, 2, 3)]
    for k in (1, 2, 3):
        beneath = beneath + jnp.where(plane >= k, got[k - 1], 0.0)
        total = total + got[k - 1]

    species = jnp.arange(LANES, dtype=jnp.int32) % KINDS
    taken = jnp.concatenate([participant_indices[0], participant_indices[1, PHOTON:]])
    g2 = (taken[:, None] == species[None, :]).astype(BF16)
    rows = jnp.arange(80, dtype=jnp.int32)[:, None]
    made = (participant_indices[2][None, :] == rows).astype(F32) + (
        participant_indices[3][None, :] == rows
    ).astype(F32)
    exo_hi = lax.reduce_precision(exothermic_energy, 8, 7)
    exo_lo = exothermic_energy - exo_hi
    pg = jnp.where(rows == 64, exo_hi[None, :], jnp.where(rows == 65, exo_lo[None, :], made))
    pg = jnp.concatenate([pg, pg], axis=1).astype(BF16)
    rows = rows[:KINDS]
    lt = jnp.concatenate(
        [participant_indices[0, PHOTON:], participant_indices[1, PHOTON:]]
    )[None, :] == rows
    lt = jnp.concatenate([lt, lt], axis=1).astype(BF16)
    lp = participant_indices[0, :PHOTON][None, :] == rows
    lp = jnp.concatenate([lp, lp], axis=1).astype(BF16)
    op_hi = lax.reduce_precision(opacity_area, 8, 7)
    ost = jnp.concatenate([op_hi, op_hi, opacity_area - op_hi], axis=1).astype(BF16)
    k_in = (jnp.arange(2 * LANES, dtype=jnp.int32) % LANES)[:, None]
    k_out = jnp.arange(LANES, dtype=jnp.int32)[None, :]
    uu = jnp.where(k_in < k_out, 1.0, jnp.where(k_in == k_out, 0.5, 0.0)).astype(BF16)
    cols = jnp.stack([arrhenius_coefficient, arrhenius_barrier * (-LOG2E)], axis=1)

    n_new, temp_new, up, dn, zs = pl.pallas_call(
        chemistry_kernel,
        out_shape=(
            sds(TILES, KINDS, LANES), sds(TILES, LANES), sds(520, LANES), sds(520, LANES),
            sds(KINDS, LANES),
        ),
        in_specs=[SM, SM, SM] + [VM] * 17,
        out_specs=(VM,) * 5,
        scratch_shapes=[
            pltpu.VMEM((TILES * KINDS, LANES), F32),
            pltpu.VMEM((TILES, PHOTON, LANES), F32),
            pltpu.VMEM((TILES, KINDS, LANES), F32),
            pltpu.VMEM((MAXD, KINDS, LANES), F32),
            pltpu.VMEM((8, LANES), F32),
        ],
        name="chemistry",
    )(
        jnp.stack([gx, gz]).astype(F32), illumination, demanding_patches.reshape(MAXD),
        n2, temp, v, xown, xpay, beneath, total, zown, zpay,
        ost, uu, g2, pg, lt, lp, cols, emission_loss[:, None],
    )

    low = lax.ppermute(up, "gy", around(size, 1))
    high = lax.ppermute(dn, "gy", around(size, -1))
    hx = lax.ppermute(n_new, "gx", around(gx_size, 1))
    hz = lax.ppermute(zs, "gz", around(gz_size, 1))

    out = pl.pallas_call(
        transport_kernel,
        out_shape=sds(KINDS * TILES, LANES),
        in_specs=[VM] * 8,
        out_specs=VM,
        name="transport",
    )(n_new, v, hx, xpay, low, high, hz, zpay)
    return out.reshape(KINDS, 4, 4, LANES), temp_new.reshape(4, 4, LANES)


def solution(mesh):
    field = P(None, "gx", "gy", "gz")
    return jax.shard_map(
        shards,
        mesh=mesh,
        in_specs=(field, P("gx", "gy", "gz"), field) + (P(),) * 7 + (P("gx", "gy", "gz", None),),
        out_specs=(field, P("gx", "gy", "gz")),
        check_vma=False,
    )
```

```python
import functools

import jax
import jax.numpy as jnp
from jax import lax
from jax.experimental import pallas as pl
from jax.experimental.pallas import tpu as pltpu
from jax.sharding import PartitionSpec as P

KINDS = 64
PHOTON = 128
NSUB = 8
TILES = 16
LANES = 128
MAXD = 4
LOG2E = 1.4426950408889634

F32 = jnp.float32
BF16 = jnp.bfloat16


def split(x):
    hi = x.astype(BF16)
    lo = (x - hi.astype(F32)).astype(BF16)
    return hi, lo


def dot(a, b):
    return jnp.dot(a, b, preferred_element_type=F32)


def totals_kernel(n_ref, v_ref, n2_ref, ty_ref, xpay_ref, zpay_ref):
    tiles = []
    for t in range(TILES):
        a = n_ref[pl.ds(t, KINDS, stride=TILES), :]
        n2_ref[t] = a
        tiles.append(a)
    for q in range(4):
        ty_ref[pl.ds(q * KINDS, KINDS), :] = (tiles[4 * q] + tiles[4 * q + 1]) + (
            tiles[4 * q + 2] + tiles[4 * q + 3]
        )
        xpay_ref[pl.ds(q * KINDS, KINDS), :] = (tiles[q] + tiles[q + 4]) + (
            tiles[q + 8] + tiles[q + 12]
        )
    lane = lax.broadcasted_iota(jnp.int32, (KINDS, LANES), 1)
    tz = jnp.zeros((KINDS, LANES), F32)
    for t in range(TILES):
        tz = jnp.where(lane == t, jnp.sum(tiles[t], axis=1, keepdims=True), tz)
    zpay_ref[pl.ds(0, KINDS), :] = tz
    xpay_ref[pl.ds(256, TILES), :] = v_ref[pl.ds(0, TILES), :]
    zpay_ref[pl.ds(KINDS, TILES), :] = v_ref[pl.ds(2 * TILES, TILES), :]


def stacked(x):
    hi, lo = split(x)
    return jnp.concatenate([hi, lo, hi], axis=0)


def local_kernel(
    light_ref, n2_ref, temp_ref, opt_ref, idx_ref, exo_ref, coef_ref, bar_ref, em_ref,
    ost_ref, g2_ref, pg_ref, lt_ref, lp_ref, cb_ref,
    made_ref, lost_ref, heat_ref, den_ref, na_ref, yl_ref, yu_ref, zc_ref,
):
    op_hi, op_lo = split(opt_ref[...])
    op_hi, op_lo = op_hi.astype(F32), op_lo.astype(F32)
    ost = jnp.concatenate([op_hi, op_hi, op_lo], axis=0).T.astype(BF16)
    ost_ref[...] = ost
    a, b = idx_ref[0:1, :], idx_ref[1:2, :]
    c, e = idx_ref[2:3, :], idx_ref[3:4, :]
    taken = wide([a, b[:, PHOTON:]])
    species = lax.broadcasted_iota(jnp.int32, (LANES, 384), 0) % KINDS
    hot = jnp.where(species == taken, 1.0, 0.0).astype(F32)
    g2 = jnp.concatenate([hot[:, q * 128 : (q + 1) * 128].T for q in range(3)], axis=0)
    g2 = g2.astype(BF16)
    g2_ref[...] = g2
    rows = lax.broadcasted_iota(jnp.int32, (80, 256), 0)
    made = jnp.where(rows == c, 1.0, 0.0) + jnp.where(rows == e, 1.0, 0.0)
    exo_hi, exo_lo = split(exo_ref[...])
    made = jnp.where(rows == 64, exo_hi.astype(F32), made)
    made = jnp.where(rows == 65, exo_lo.astype(F32), made)
    pg = wide([made, made]).astype(BF16)
    pg_ref[...] = pg
    rows = lax.broadcasted_iota(jnp.int32, (KINDS, 256), 0)
    lt = jnp.where(rows == wide([a[:, PHOTON:], b[:, PHOTON:]]), 1.0, 0.0)
    lt = wide([lt, lt]).astype(BF16)
    lt_ref[...] = lt
    lp = jnp.where(rows[:, :PHOTON] == a[:, :PHOTON], 1.0, 0.0)
    lp_ref[...] = wide([lp, lp]).astype(BF16)
    coef = jnp.broadcast_to(coef_ref[...], (LANES, LANES)).T
    bar = jnp.broadcast_to(bar_ref[...] * (-LOG2E), (LANES, LANES)).T
    em = jnp.broadcast_to(em_ref[...], (LANES, KINDS)).T
    cb_ref[pl.ds(0, LANES), :] = coef
    cb_ref[pl.ds(LANES, LANES), :] = bar
    cb_ref[pl.ds(2 * LANES, KINDS), :] = em
    k_in = lax.broadcasted_iota(jnp.int32, (2 * LANES, LANES), 0) % LANES
    k_out = lax.broadcasted_iota(jnp.int32, (2 * LANES, LANES), 1)
    uu = jnp.where(k_in < k_out, 1.0, jnp.where(k_in == k_out, 0.5, 0.0)).astype(BF16)
    coef, bar, em = wide([coef, coef]), wide([bar, bar]), wide([em, em])
    pgt = wide([pg[:, 128:256], pg[:, 384:512]])

    def four(i, carry):
        base = i * 4
        blk = n2_ref[pl.ds(base, 4)].reshape(256, LANES)
        zc_ref[pl.ds(i * 256, 256), :] = dot(wide(split(blk)), uu)
        tiles = [n2_ref[base + j] for j in range(4)]
        total = (tiles[0] + tiles[1]) + (tiles[2] + tiles[3])
        run = jnp.zeros_like(total)
        for p in range(2):
            a = base + 2 * p
            cols = []
            for j in (2 * p, 2 * p + 1):
                low = run + 0.5 * tiles[j]
                run = run + tiles[j]
                cols += [low, total - low]
            tau = dot(ost, stacked(wide(cols)))
            for q in range(4):
                part = light_ref[2 + q % 2] * jnp.exp2(
                    tau[:, q * 128 : (q + 1) * 128] * (-LOG2E / 128.0)
                )
                (yl_ref, yu_ref)[q % 2][a + q // 2] = part
            n = wide([tiles[2 * p], tiles[2 * p + 1]])
            temp = wide([temp_ref[pl.ds(a, 1), :], temp_ref[pl.ds(a + 1, 1), :]])
            gat = dot(g2, jnp.concatenate(split(n), axis=0))
            th = coef * jnp.exp2(bar * (1.0 / temp))
            kb = th * gat[256:384]
            ka = th * gat[128:256]
            made = dot(pgt, jnp.concatenate(split(kb * gat[128:256]), axis=0))
            lost = 1.0 + dot(
                lt, jnp.concatenate(split(jnp.concatenate([kb, ka], axis=0)), axis=0)
            )
            heat = made[64:65] + made[65:66]
            den = 1.0 + jnp.sum(em * n, axis=0, keepdims=True)
            for q in range(2):
                cut = slice(q * LANES, (q + 1) * LANES)
                made_ref[a + q] = made[:64, cut]
                lost_ref[a + q] = lost[:, cut]
                na_ref[a + q] = gat[:128, cut]
                heat_ref[pl.ds(a + q, 1), :] = heat[:, cut]
                den_ref[pl.ds(a + q, 1), :] = den[:, cut]
        return carry

    lax.fori_loop(0, 4, four, 0)


def wide(parts):
    return jnp.concatenate(parts, axis=1)


def early_kernel(light_ref, n2_ref, zc_ref, xown_ref, xpay_ref, zown_ref, zpay_ref, ost_ref, pe_ref):
    gx = lax.axis_index("gx").astype(F32)
    gz = lax.axis_index("gz").astype(F32)
    ost = ost_ref[...]
    zsum = zown_ref[pl.ds(0, KINDS), :] + zpay_ref[pl.ds(0, KINDS), :]
    zlow = gz * zpay_ref[pl.ds(0, KINDS), :]
    runx = [gx * xpay_ref[pl.ds(q * KINDS, KINDS), :] for q in range(4)]
    for i in range(4):
        for j in range(4):
            t = i * 4 + j
            n = n2_ref[t]
            xl = runx[j] + 0.5 * n
            runx[j] = runx[j] + n
            zl = zc_ref[pl.ds(t * KINDS, KINDS), :] + zlow[:, t : t + 1]
            xsum = xown_ref[pl.ds(j * KINDS, KINDS), :] + xpay_ref[pl.ds(j * KINDS, KINDS), :]
            tau = dot(ost, stacked(wide([xl, xsum - xl, zl, zsum[:, t : t + 1] - zl])))
            ph = None
            for q in range(4):
                size, d = ((8.0, 0), (8.0, 1), (256.0, 4), (256.0, 5))[q]
                part = light_ref[d] * jnp.exp2(tau[:, q * 128 : (q + 1) * 128] * (-LOG2E / size))
                ph = part if q == 0 else ph + part
            pe_ref[t] = ph


def chemistry_kernel(
    listed_ref,
    n2_ref, temp_ref, v_ref, ty_ref, below_ref, total_ref, last_ref, pe_ref,
    ost_ref, g2_ref, pg_ref, lt_ref, lp_ref, cb_ref,
    made_ref, lost_ref, heat_ref, den_ref, na_ref, yl_ref, yu_ref,
    n_out, temp_out, up_out, dn_out, z_out,
    ph_ref, ll_ref, cur_ref, curt_ref,
):
    upper = jnp.where(lax.axis_index("gy") >= 16, 1.0, 0.0).astype(F32)
    ost = ost_ref[...]
    for i in range(4):
        cut = pl.ds(i * KINDS, KINDS)
        last = last_ref[cut, :]
        below = below_ref[cut, :] + upper * last
        above = (total_ref[cut, :] + last) - below - ty_ref[cut, :]
        far = jnp.exp2(dot(ost, stacked(wide([below, above]))) * (-LOG2E / 128.0))
        for j in range(4):
            t = i * 4 + j
            ph_ref[t] = pe_ref[t] + (yl_ref[t] * far[:, :LANES] + yu_ref[t] * far[:, LANES:])

    lp = lp_ref[...]
    pgp = wide([pg_ref[:, 0:128], pg_ref[:, 256:384]])

    def quiet(c, carry):
        base = c * 4
        for p in range(2):
            a = base + 2 * p
            ph = wide([ph_ref[a], ph_ref[a + 1]])
            ll = dot(lp, jnp.concatenate(split(ph), axis=0))
            na = wide([na_ref[a], na_ref[a + 1]])
            made = dot(pgp, jnp.concatenate(split(ph * na), axis=0))
            heat = made[64:65] + made[65:66]
            for q in range(2):
                cut = slice(q * LANES, (q + 1) * LANES)
                ll_ref[a + q] = ll[:, cut]
                n_out[a + q] = (n2_ref[a + q] + (made_ref[a + q] + made[:64, cut])) / (
                    lost_ref[a + q] + ll[:, cut]
                )
                row = pl.ds(a + q, 1)
                temp_out[row, :] = (temp_ref[row, :] + (heat_ref[row, :] + heat[:, cut])) / (
                    den_ref[row, :]
                )
        return carry

    lax.fori_loop(0, 4, quiet, 0)

    pick = [jnp.minimum(listed_ref[m], TILES - 1) for m in range(MAXD)]
    for m in range(MAXD):
        cur_ref[m] = n2_ref[pick[m]]
        curt_ref[pl.ds(m, 1), :] = temp_ref[pl.ds(pick[m], 1), :]
    g2, pg, lt = g2_ref[...], pg_ref[...], lt_ref[...]
    coef = cb_ref[pl.ds(0, LANES), :]
    bar = cb_ref[pl.ds(LANES, LANES), :]
    em = cb_ref[pl.ds(2 * LANES, KINDS), :]
    coef, bar, em = wide([coef, coef]), wide([bar, bar]), wide([em, em])
    h = 1.0 / NSUB

    def substep(s, carry):
        for p in range(2):
            a, b = 2 * p, 2 * p + 1
            n = wide([cur_ref[a], cur_ref[b]])
            temp = wide([curt_ref[a : a + 1, :], curt_ref[b : b + 1, :]])
            ph = wide([ph_ref[pick[a]], ph_ref[pick[b]]])
            ll = wide([ll_ref[pick[a]], ll_ref[pick[b]]])
            th = coef * jnp.exp2(bar * (1.0 / temp))
            gat = dot(g2, jnp.concatenate(split(n), axis=0))
            kb = th * gat[256:384]
            ka = th * gat[128:256]
            rate = jnp.concatenate([ph * gat[:128], kb * gat[128:256]], axis=0)
            rem = jnp.concatenate([kb, ka], axis=0)
            made = dot(pg, jnp.concatenate(split(rate), axis=0))
            lost = dot(lt, jnp.concatenate(split(rem), axis=0)) + ll
            heat = made[64:65] + made[65:66]
            cool = jnp.sum(em * n, axis=0, keepdims=True)
            nn = (n + h * made[:64]) / (1.0 + h * lost)
            tt = (temp + h * heat) / (1.0 + h * cool)
            cur_ref[a] = nn[:, :LANES]
            cur_ref[b] = nn[:, LANES:]
            curt_ref[a : a + 1, :] = tt[:, :LANES]
            curt_ref[b : b + 1, :] = tt[:, LANES:]
        return carry

    lax.fori_loop(0, NSUB, substep, 0)

    for m in range(MAXD):

        @pl.when(listed_ref[m] < TILES)
        def _():
            n_out[pick[m]] = cur_ref[m]
            temp_out[pl.ds(pick[m], 1), :] = curt_ref[m : m + 1, :]

    lane = lax.broadcasted_iota(jnp.int32, (KINDS, LANES), 1)
    zp = jnp.zeros((KINDS, LANES), F32)
    up_out[pl.ds(512, 8), :] = jnp.zeros((8, LANES), F32)
    dn_out[pl.ds(512, 8), :] = jnp.zeros((8, LANES), F32)
    for i in range(4):
        for j in range(4):
            t = i * 4 + j
            u = n_out[t]
            zp = jnp.where(lane // 8 == t, pltpu.roll(u, (8 * t + 4) % LANES, 1), zp)
            if j < 2:
                dn_out[pl.ds((j * 4 + i) * KINDS, KINDS), :] = u
            else:
                up_out[pl.ds(((j - 2) * 4 + i) * KINDS, KINDS), :] = u
        up_out[pl.ds(512 + i, 1), :] = v_ref[pl.ds(TILES + i * 4 + 3, 1), :]
        dn_out[pl.ds(512 + i, 1), :] = v_ref[pl.ds(TILES + i * 4, 1), :]
    z_out[...] = zp


def flux(face, um1, u, up1, up2):
    state = jnp.where(face > 0, 1.5 * u - 0.5 * um1, 1.5 * up1 - 0.5 * up2)
    return face * state


def inner_kernel(n_ref, v_ref, hx_ref, xpay_ref, acc_ref):
    lane = lax.broadcasted_iota(jnp.int32, (KINDS, LANES), 1)
    edge = jnp.logical_or(lane < 2, lane >= LANES - 2)

    def x_u(i, j):
        if 0 <= i < 4:
            return n_ref[i * 4 + j]
        return hx_ref[(i % 4) * 4 + j]

    def x_v(i, j):
        if 0 <= i < 4:
            return v_ref[i * 4 + j : i * 4 + j + 1, :]
        r = 256 + (i % 4) * 4 + j
        return xpay_ref[r : r + 1, :]

    def x_flux(i, j):
        face = 0.5 * (x_v(i, j) + x_v(i + 1, j))
        return flux(face, x_u(i - 1, j), x_u(i, j), x_u(i + 1, j), x_u(i + 2, j))

    xf = [x_flux(-1, j) for j in range(4)]
    for i in range(4):
        for j in range(4):
            t = i * 4 + j
            u = n_ref[t]
            top = x_flux(i, j)
            change = top - xf[j]
            xf[j] = top
            vz = v_ref[32 + t : 33 + t, :]
            face = 0.5 * (vz + pltpu.roll(vz, LANES - 1, 1))
            fz = flux(
                face,
                pltpu.roll(u, 1, 1),
                u,
                pltpu.roll(u, LANES - 1, 1),
                pltpu.roll(u, LANES - 2, 1),
            )
            change = change + jnp.where(edge, 0.0, fz - pltpu.roll(fz, 1, 1))
            acc_ref[t] = u - 0.25 * change


def outer_kernel(n_ref, acc_ref, v_ref, lo_ref, hi_ref, zs_ref, hz_ref, zpay_ref, out_ref):
    lane = lax.broadcasted_iota(jnp.int32, (KINDS, LANES), 1)
    lane1 = lax.broadcasted_iota(jnp.int32, (1, LANES), 1)
    edge = jnp.logical_or(lane < 2, lane >= LANES - 2)

    vown = jnp.zeros((1, LANES), F32)
    vpart = jnp.zeros((1, LANES), F32)
    for t in range(TILES):
        here = lane1 // 8 == t
        vown = jnp.where(here, pltpu.roll(v_ref[32 + t : 33 + t, :], (8 * t + 4) % LANES, 1), vown)
        vpart = jnp.where(
            here, pltpu.roll(zpay_ref[64 + t : 65 + t, :], (8 * t + 4) % LANES, 1), vpart
        )
    own, part = zs_ref[...], hz_ref[...]
    high = lane % 8 < 4
    high1 = lane1 % 8 < 4
    top, tv = jnp.where(high, own, part), jnp.where(high1, vown, vpart)
    low, lv = jnp.where(high, part, own), jnp.where(high1, vpart, vown)

    def line(u, v):
        face = 0.5 * (v + pltpu.roll(v, LANES - 1, 1))
        f = flux(
            face, pltpu.roll(u, 1, 1), u, pltpu.roll(u, LANES - 1, 1), pltpu.roll(u, LANES - 2, 1)
        )
        return f - pltpu.roll(f, 1, 1)

    packed = jnp.where(high, line(top, tv), line(low, lv))

    def y_u(i, j):
        if j < 0:
            return lo_ref[pl.ds(((j + 2) * 4 + i) * KINDS, KINDS), :]
        if j > 3:
            return hi_ref[pl.ds(((j - 4) * 4 + i) * KINDS, KINDS), :]
        return n_ref[i * 4 + j]

    def y_v(i, j):
        if j < 0:
            return lo_ref[512 + i : 513 + i, :]
        if j > 3:
            return hi_ref[512 + i : 513 + i, :]
        return v_ref[16 + i * 4 + j : 17 + i * 4 + j, :]

    def y_flux(i, j):
        face = 0.5 * (y_v(i, j) + y_v(i, j + 1))
        return flux(face, y_u(i, j - 1), y_u(i, j), y_u(i, j + 1), y_u(i, j + 2))

    for i in range(4):
        yf = y_flux(i, -1)
        for j in range(4):
            t = i * 4 + j
            up = y_flux(i, j)
            zfix = jnp.where(edge, pltpu.roll(packed, (LANES - (8 * t + 4)) % LANES, 1), 0.0)
            out_ref[pl.ds(t, KINDS, stride=TILES), :] = acc_ref[t] - 0.25 * ((up - yf) + zfix)
            yf = up


def hbm(*shape):
    return jax.ShapeDtypeStruct(shape, F32)


def vm(*shape, dtype=F32):
    return pltpu.VMEM(shape, dtype)


VM = pl.BlockSpec(memory_space=pltpu.VMEM)
SM = pl.BlockSpec(memory_space=pltpu.SMEM)


def near(x):
    return pltpu.with_memory_space_constraint(x, pltpu.VMEM)


def call(kernel, name, out_shape, scalars, inputs, scratch=()):
    return pl.pallas_call(
        kernel,
        out_shape=out_shape,
        in_specs=[SM] * len(scalars) + [VM] * len(inputs),
        out_specs=jax.tree.map(lambda _: VM, out_shape),
        scratch_shapes=scratch,
        compiler_params=pltpu.CompilerParams(vmem_limit_bytes=16 * 1024 * 1024),
        name=name,
    )(*scalars, *inputs)


def shards(
    number_densities, kinetic_kelvin, flow_vector, opacity_area, illumination,
    arrhenius_coefficient, arrhenius_barrier, exothermic_energy, emission_loss,
    participant_indices, demanding_patches,
):
    n = number_densities.reshape(KINDS * TILES, LANES)
    v = flow_vector.reshape(3 * TILES, LANES)
    temp = kinetic_kelvin.reshape(TILES, LANES)
    scope = jax.named_scope
    with scope("k_totals"):
        n2, ty, xown, zown = call(
            totals_kernel, "totals",
            (vm(TILES, KINDS, LANES), vm(256, LANES), vm(272, LANES), vm(80, LANES)),
            [], [n, v],
        )

    gy = lax.axis_index("gy")
    size = lax.axis_size("gy")
    around = lambda count, by: [(a, (a + by) % count) for a in range(count)]

    rounds = [
        ("round_x", gy % 2 >= 1, lambda a: a ^ 1),
        ("round_y0", (gy // 2) % 2 >= 1, lambda a: a ^ 2),
        ("round_y1", (gy // 2) % 4 >= 2, lambda a: (a // 8) * 8 + (3 - (a // 2) % 4) * 2 + a % 2),
        ("round_z0", (gy // 8) % 2 >= 1, lambda a: a ^ 8),
        ("round_z1", None, lambda a: (3 - a // 8) * 8 + a % 8),
    ]
    below, total = jnp.zeros_like(ty), ty
    for name, later, to in rounds:
        with scope(name):
            last = lax.ppermute(total, "gy", [(a, to(a)) for a in range(size)])
        if name == "round_x":
            with scope("pay_x"):
                xpay = near(lax.ppermute(xown, "gx", around(lax.axis_size("gx"), 1)))
            with scope("pay_z"):
                zpay = near(lax.ppermute(zown, "gz", around(lax.axis_size("gz"), 1)))
        if later is not None:
            below = below + jnp.where(later, last, 0.0)
            total = total + last
    below, total, last = near(below), near(total), near(last)

    big = (TILES, PHOTON, LANES)
    mid = (TILES, KINDS, LANES)
    with scope("k_local"):
        (ost, g2, pg, lt, lp, cb, made, lost, heat, den, na, yl, yu, zc) = call(
            local_kernel, "local",
            (
                vm(128, 192, dtype=BF16), vm(384, 128, dtype=BF16), vm(80, 512, dtype=BF16),
                vm(64, 512, dtype=BF16), vm(64, 256, dtype=BF16), vm(320, LANES),
                vm(*mid), vm(*mid), vm(TILES, LANES), vm(TILES, LANES), vm(*big), vm(*big),
                vm(*big), vm(TILES * KINDS, LANES),
            ),
            [illumination],
            [
                n2, temp, opacity_area.T, participant_indices, exothermic_energy[None],
                arrhenius_coefficient[None], arrhenius_barrier[None], emission_loss[None],
            ],
        )
    with scope("k_early"):
        pe = call(
            early_kernel, "early", vm(*big), [illumination],
            [n2, zc, xown, xpay, zown, zpay, ost],
        )
    with scope("k_chem"):
        n_new, temp_new, up, dn, zs = call(
            chemistry_kernel, "chemistry",
            (vm(*mid), hbm(TILES, LANES), vm(520, LANES), vm(520, LANES), vm(KINDS, LANES)),
            [demanding_patches.reshape(MAXD)],
            [
                n2, temp, v, ty, below, total, last, pe, ost, g2, pg, lt, lp, cb,
                made, lost, heat, den, na, yl, yu,
            ],
            [
                pltpu.VMEM(big, F32), pltpu.VMEM(mid, F32),
                pltpu.VMEM((MAXD, KINDS, LANES), F32), pltpu.VMEM((8, LANES), F32),
            ],
        )

    with scope("halo_up"):
        low = near(lax.ppermute(up, "gy", around(size, 1)))
    with scope("halo_dn"):
        high = near(lax.ppermute(dn, "gy", around(size, -1)))
    with scope("halo_x"):
        hx = near(lax.ppermute(n_new, "gx", around(lax.axis_size("gx"), 1)))
    with scope("halo_z"):
        hz = near(lax.ppermute(zs, "gz", around(lax.axis_size("gz"), 1)))
    with scope("k_inner"):
        acc = call(inner_kernel, "inner", vm(*mid), [], [n_new, v, hx, xpay])
    with scope("k_outer"):
        out = call(
            outer_kernel, "outer", hbm(KINDS * TILES, LANES), [],
            [n_new, acc, v, low, high, zs, hz, zpay],
        )
    return out.reshape(KINDS, 4, 4, LANES), temp_new.reshape(4, 4, LANES)


def solution(mesh):
    field = P(None, "gx", "gy", "gz")
    return jax.shard_map(
        shards,
        mesh=mesh,
        in_specs=(field, P("gx", "gy", "gz"), field) + (P(),) * 7 + (P("gx", "gy", "gz", None),),
        out_specs=(field, P("gx", "gy", "gz")),
        check_vma=False,
    )
```

```python
import functools

import jax
import jax.numpy as jnp
from jax import lax
from jax.experimental import pallas as pl
from jax.experimental.pallas import tpu as pltpu
from jax.sharding import PartitionSpec as P


KINDS = 64
PHOTON = 128
NSUB = 8
TILES = 16
LANES = 128
MAXD = 4
LOG2E = 1.4426950408889634

F32 = jnp.float32
BF16 = jnp.bfloat16


def split(x):
    hi = x.astype(BF16)
    lo = (x - hi.astype(F32)).astype(BF16)
    return hi, lo


def dot(a, b):
    return jnp.dot(a, b, preferred_element_type=F32)


def totals_kernel(n_ref, n2_ref, ty_ref, xpay_ref, zpay_ref):
    tiles = []
    for t in range(TILES):
        a = n_ref[pl.ds(t, KINDS, stride=TILES), :]
        n2_ref[t] = a
        tiles.append(a)
    for q in range(4):
        ty_ref[pl.ds(q * KINDS, KINDS), :] = (tiles[4 * q] + tiles[4 * q + 1]) + (
            tiles[4 * q + 2] + tiles[4 * q + 3]
        )
        xpay_ref[pl.ds(q * KINDS, KINDS), :] = (tiles[q] + tiles[q + 4]) + (
            tiles[q + 8] + tiles[q + 12]
        )
    lane = lax.broadcasted_iota(jnp.int32, (KINDS, LANES), 1)
    tz = jnp.zeros((KINDS, LANES), F32)
    for t in range(TILES):
        tz = jnp.where(lane == t, jnp.sum(tiles[t], axis=1, keepdims=True), tz)
    zpay_ref[...] = tz


def combine_kernel(block, count, least, last_ref, total_ref, *refs):
    below_ref, (below_out, total_out) = refs[:-2], refs[-2:]
    here = lax.rem(lax.div(lax.axis_index("gy"), block), count)
    later = jnp.where(here >= least, 1.0, 0.0).astype(F32)
    last = last_ref[...]
    total_out[...] = total_ref[...] + last
    below = later * last
    below_out[...] = below + below_ref[0][...] if below_ref else below


def stacked(x):
    hi, lo = split(x)
    return jnp.concatenate([hi, lo, hi], axis=0)


def local_kernel(
    light_ref, n2_ref, temp_ref, opt_ref, idx_ref, exo_ref, coef_ref, bar_ref, em_ref,
    ost_ref, g2_ref, pg_ref, lt_ref, lp_ref, cb_ref,
    made_ref, lost_ref, heat_ref, den_ref, na_ref, yl_ref, yu_ref, zc_ref,
):
    op_hi, op_lo = split(opt_ref[...])
    op_hi, op_lo = op_hi.astype(F32), op_lo.astype(F32)
    ost = jnp.concatenate([op_hi, op_hi, op_lo], axis=0).T.astype(BF16)
    ost_ref[...] = ost
    a, b = idx_ref[0:1, :], idx_ref[1:2, :]
    c, e = idx_ref[2:3, :], idx_ref[3:4, :]
    taken = wide([a, b[:, PHOTON:]])
    species = lax.broadcasted_iota(jnp.int32, (LANES, 384), 0) % KINDS
    hot = jnp.where(species == taken, 1.0, 0.0).astype(F32)
    g2 = jnp.concatenate([hot[:, q * 128 : (q + 1) * 128].T for q in range(3)], axis=0)
    g2 = g2.astype(BF16)
    g2_ref[...] = g2
    rows = lax.broadcasted_iota(jnp.int32, (80, 256), 0)
    made = jnp.where(rows == c, 1.0, 0.0) + jnp.where(rows == e, 1.0, 0.0)
    exo_hi, exo_lo = split(exo_ref[...])
    made = jnp.where(rows == 64, exo_hi.astype(F32), made)
    made = jnp.where(rows == 65, exo_lo.astype(F32), made)
    pg = wide([made, made]).astype(BF16)
    pg_ref[...] = pg
    rows = lax.broadcasted_iota(jnp.int32, (KINDS, 256), 0)
    lt = jnp.where(rows == wide([a[:, PHOTON:], b[:, PHOTON:]]), 1.0, 0.0)
    lt = wide([lt, lt]).astype(BF16)
    lt_ref[...] = lt
    lp = jnp.where(rows[:, :PHOTON] == a[:, :PHOTON], 1.0, 0.0)
    lp_ref[...] = wide([lp, lp]).astype(BF16)
    coef = jnp.broadcast_to(coef_ref[...], (LANES, LANES)).T
    bar = jnp.broadcast_to(bar_ref[...] * (-LOG2E), (LANES, LANES)).T
    em = jnp.broadcast_to(em_ref[...], (LANES, KINDS)).T
    cb_ref[pl.ds(0, LANES), :] = coef
    cb_ref[pl.ds(LANES, LANES), :] = bar
    cb_ref[pl.ds(2 * LANES, KINDS), :] = em
    k_in = lax.broadcasted_iota(jnp.int32, (2 * LANES, LANES), 0) % LANES
    k_out = lax.broadcasted_iota(jnp.int32, (2 * LANES, LANES), 1)
    uu = jnp.where(k_in < k_out, 1.0, jnp.where(k_in == k_out, 0.5, 0.0)).astype(BF16)
    coef, bar, em = wide([coef, coef]), wide([bar, bar]), wide([em, em])
    pgt = wide([pg[:, 128:256], pg[:, 384:512]])

    def four(i, carry):
        base = i * 4
        blk = n2_ref[pl.ds(base, 4)].reshape(256, LANES)
        zc_ref[pl.ds(i * 256, 256), :] = dot(wide(split(blk)), uu)
        tiles = [n2_ref[base + j] for j in range(4)]
        total = (tiles[0] + tiles[1]) + (tiles[2] + tiles[3])
        run = jnp.zeros_like(total)
        for p in range(2):
            a = base + 2 * p
            cols = []
            for j in (2 * p, 2 * p + 1):
                low = run + 0.5 * tiles[j]
                run = run + tiles[j]
                cols += [low, total - low]
            tau = dot(ost, stacked(wide(cols)))
            for q in range(4):
                part = light_ref[2 + q % 2] * jnp.exp2(
                    tau[:, q * 128 : (q + 1) * 128] * (-LOG2E / 128.0)
                )
                (yl_ref, yu_ref)[q % 2][a + q // 2] = part
            n = wide([tiles[2 * p], tiles[2 * p + 1]])
            temp = wide([temp_ref[pl.ds(a, 1), :], temp_ref[pl.ds(a + 1, 1), :]])
            gat = dot(g2, jnp.concatenate(split(n), axis=0))
            th = coef * jnp.exp2(bar * (1.0 / temp))
            kb = th * gat[256:384]
            ka = th * gat[128:256]
            made = dot(pgt, jnp.concatenate(split(kb * gat[128:256]), axis=0))
            lost = 1.0 + dot(
                lt, jnp.concatenate(split(jnp.concatenate([kb, ka], axis=0)), axis=0)
            )
            heat = made[64:65] + made[65:66]
            den = 1.0 + jnp.sum(em * n, axis=0, keepdims=True)
            for q in range(2):
                cut = slice(q * LANES, (q + 1) * LANES)
                made_ref[a + q] = made[:64, cut]
                lost_ref[a + q] = lost[:, cut]
                na_ref[a + q] = gat[:128, cut]
                heat_ref[pl.ds(a + q, 1), :] = heat[:, cut]
                den_ref[pl.ds(a + q, 1), :] = den[:, cut]
        return carry

    lax.fori_loop(0, 4, four, 0)


def wide(parts):
    return jnp.concatenate(parts, axis=1)


def early_kernel(light_ref, n2_ref, zc_ref, xown_ref, xpay_ref, zown_ref, zpay_ref, ost_ref, pe_ref):
    gx = lax.axis_index("gx").astype(F32)
    gz = lax.axis_index("gz").astype(F32)
    ost = ost_ref[...]
    zsum = zown_ref[pl.ds(0, KINDS), :] + zpay_ref[pl.ds(0, KINDS), :]
    zlow = gz * zpay_ref[pl.ds(0, KINDS), :]
    runx = [gx * xpay_ref[pl.ds(q * KINDS, KINDS), :] for q in range(4)]
    for i in range(4):
        for j in range(4):
            t = i * 4 + j
            n = n2_ref[t]
            xl = runx[j] + 0.5 * n
            runx[j] = runx[j] + n
            zl = zc_ref[pl.ds(t * KINDS, KINDS), :] + zlow[:, t : t + 1]
            xsum = xown_ref[pl.ds(j * KINDS, KINDS), :] + xpay_ref[pl.ds(j * KINDS, KINDS), :]
            tau = dot(ost, stacked(wide([xl, xsum - xl, zl, zsum[:, t : t + 1] - zl])))
            ph = None
            for q in range(4):
                size, d = ((8.0, 0), (8.0, 1), (256.0, 4), (256.0, 5))[q]
                part = light_ref[d] * jnp.exp2(tau[:, q * 128 : (q + 1) * 128] * (-LOG2E / size))
                ph = part if q == 0 else ph + part
            pe_ref[t] = ph


def chemistry_kernel(
    listed_ref,
    n2_ref, temp_ref, v_ref, ty_ref, below_ref, total_ref, last_ref, pe_ref,
    ost_ref, g2_ref, pg_ref, lt_ref, lp_ref, cb_ref,
    made_ref, lost_ref, heat_ref, den_ref, na_ref, yl_ref, yu_ref,
    n_out, temp_out, up_out, dn_out, z_out,
    ph_ref, ll_ref, cur_ref, curt_ref,
):
    upper = jnp.where(lax.axis_index("gy") >= 16, 1.0, 0.0).astype(F32)
    ost = ost_ref[...]
    for i in range(4):
        cut = pl.ds(i * KINDS, KINDS)
        last = last_ref[cut, :]
        below = below_ref[cut, :] + upper * last
        above = (total_ref[cut, :] + last) - below - ty_ref[cut, :]
        far = jnp.exp2(dot(ost, stacked(wide([below, above]))) * (-LOG2E / 128.0))
        for j in range(4):
            t = i * 4 + j
            ph_ref[t] = pe_ref[t] + (yl_ref[t] * far[:, :LANES] + yu_ref[t] * far[:, LANES:])

    lp = lp_ref[...]
    pgp = wide([pg_ref[:, 0:128], pg_ref[:, 256:384]])

    def quiet(c, carry):
        base = c * 4
        for p in range(2):
            a = base + 2 * p
            ph = wide([ph_ref[a], ph_ref[a + 1]])
            ll = dot(lp, jnp.concatenate(split(ph), axis=0))
            na = wide([na_ref[a], na_ref[a + 1]])
            made = dot(pgp, jnp.concatenate(split(ph * na), axis=0))
            heat = made[64:65] + made[65:66]
            for q in range(2):
                cut = slice(q * LANES, (q + 1) * LANES)
                ll_ref[a + q] = ll[:, cut]
                n_out[pl.ds(pl.multiple_of((a + q) * KINDS, KINDS), KINDS), :] = (n2_ref[a + q] + (made_ref[a + q] + made[:64, cut])) / (
                    lost_ref[a + q] + ll[:, cut]
                )
                row = pl.ds(a + q, 1)
                temp_out[row, :] = (temp_ref[row, :] + (heat_ref[row, :] + heat[:, cut])) / (
                    den_ref[row, :]
                )
        return carry

    lax.fori_loop(0, 4, quiet, 0)

    pick = [jnp.minimum(listed_ref[m], TILES - 1) for m in range(MAXD)]
    for m in range(MAXD):
        cur_ref[m] = n2_ref[pick[m]]
        curt_ref[pl.ds(m, 1), :] = temp_ref[pl.ds(pick[m], 1), :]
    g2, pg, lt = g2_ref[...], pg_ref[...], lt_ref[...]
    coef = cb_ref[pl.ds(0, LANES), :]
    bar = cb_ref[pl.ds(LANES, LANES), :]
    em = cb_ref[pl.ds(2 * LANES, KINDS), :]
    coef, bar, em = wide([coef, coef]), wide([bar, bar]), wide([em, em])
    h = 1.0 / NSUB

    def substep(s, carry):
        for p in range(2):
            a, b = 2 * p, 2 * p + 1
            n = wide([cur_ref[a], cur_ref[b]])
            temp = wide([curt_ref[a : a + 1, :], curt_ref[b : b + 1, :]])
            ph = wide([ph_ref[pick[a]], ph_ref[pick[b]]])
            ll = wide([ll_ref[pick[a]], ll_ref[pick[b]]])
            th = coef * jnp.exp2(bar * (1.0 / temp))
            gat = dot(g2, jnp.concatenate(split(n), axis=0))
            kb = th * gat[256:384]
            ka = th * gat[128:256]
            rate = jnp.concatenate([ph * gat[:128], kb * gat[128:256]], axis=0)
            rem = jnp.concatenate([kb, ka], axis=0)
            made = dot(pg, jnp.concatenate(split(rate), axis=0))
            lost = dot(lt, jnp.concatenate(split(rem), axis=0)) + ll
            heat = made[64:65] + made[65:66]
            cool = jnp.sum(em * n, axis=0, keepdims=True)
            nn = (n + h * made[:64]) / (1.0 + h * lost)
            tt = (temp + h * heat) / (1.0 + h * cool)
            cur_ref[a] = nn[:, :LANES]
            cur_ref[b] = nn[:, LANES:]
            curt_ref[a : a + 1, :] = tt[:, :LANES]
            curt_ref[b : b + 1, :] = tt[:, LANES:]
        return carry

    lax.fori_loop(0, NSUB, substep, 0)

    for m in range(MAXD):

        @pl.when(listed_ref[m] < TILES)
        def _():
            n_out[pl.ds(pl.multiple_of(pick[m] * KINDS, KINDS), KINDS), :] = cur_ref[m]
            temp_out[pl.ds(pick[m], 1), :] = curt_ref[m : m + 1, :]

    lane = lax.broadcasted_iota(jnp.int32, (KINDS, LANES), 1)
    zp = jnp.zeros((KINDS, LANES), F32)
    up_out[pl.ds(512, 8), :] = jnp.zeros((8, LANES), F32)
    dn_out[pl.ds(512, 8), :] = jnp.zeros((8, LANES), F32)
    for i in range(4):
        for j in range(4):
            t = i * 4 + j
            u = n_out[pl.ds(t * KINDS, KINDS), :]
            zp = jnp.where(lane // 8 == t, pltpu.roll(u, (8 * t + 4) % LANES, 1), zp)
            if j < 2:
                dn_out[pl.ds((j * 4 + i) * KINDS, KINDS), :] = u
            else:
                up_out[pl.ds(((j - 2) * 4 + i) * KINDS, KINDS), :] = u
        up_out[pl.ds(512 + i, 1), :] = v_ref[pl.ds(TILES + i * 4 + 3, 1), :]
        dn_out[pl.ds(512 + i, 1), :] = v_ref[pl.ds(TILES + i * 4, 1), :]
    z_out[pl.ds(0, KINDS), :] = zp
    n_out[pl.ds(1024, TILES), :] = v_ref[pl.ds(0, TILES), :]
    z_out[pl.ds(KINDS, TILES), :] = v_ref[pl.ds(2 * TILES, TILES), :]


def flux(face, um1, u, up1, up2):
    state = jnp.where(face > 0, 1.5 * u - 0.5 * um1, 1.5 * up1 - 0.5 * up2)
    return face * state


def inner_kernel(n_ref, v_ref, hx_ref, acc_ref):
    lane = lax.broadcasted_iota(jnp.int32, (KINDS, LANES), 1)
    edge = jnp.logical_or(lane < 2, lane >= LANES - 2)

    def x_u(i, j):
        if 0 <= i < 4:
            return n_ref[pl.ds((i * 4 + j) * KINDS, KINDS), :]
        return hx_ref[pl.ds(((i % 4) * 4 + j) * KINDS, KINDS), :]

    def x_v(i, j):
        if 0 <= i < 4:
            return v_ref[i * 4 + j : i * 4 + j + 1, :]
        r = 1024 + (i % 4) * 4 + j
        return hx_ref[r : r + 1, :]

    def x_flux(i, j):
        face = 0.5 * (x_v(i, j) + x_v(i + 1, j))
        return flux(face, x_u(i - 1, j), x_u(i, j), x_u(i + 1, j), x_u(i + 2, j))

    xf = [x_flux(-1, j) for j in range(4)]
    for i in range(4):
        for j in range(4):
            t = i * 4 + j
            u = n_ref[pl.ds(t * KINDS, KINDS), :]
            top = x_flux(i, j)
            change = top - xf[j]
            xf[j] = top
            vz = v_ref[32 + t : 33 + t, :]
            face = 0.5 * (vz + pltpu.roll(vz, LANES - 1, 1))
            fz = flux(
                face,
                pltpu.roll(u, 1, 1),
                u,
                pltpu.roll(u, LANES - 1, 1),
                pltpu.roll(u, LANES - 2, 1),
            )
            change = change + jnp.where(edge, 0.0, fz - pltpu.roll(fz, 1, 1))
            acc_ref[t] = u - 0.25 * change


def outer_kernel(n_ref, acc_ref, v_ref, lo_ref, hi_ref, zs_ref, hz_ref, out_ref):
    lane = lax.broadcasted_iota(jnp.int32, (KINDS, LANES), 1)
    lane1 = lax.broadcasted_iota(jnp.int32, (1, LANES), 1)
    edge = jnp.logical_or(lane < 2, lane >= LANES - 2)

    vown = jnp.zeros((1, LANES), F32)
    vpart = jnp.zeros((1, LANES), F32)
    for t in range(TILES):
        here = lane1 // 8 == t
        vown = jnp.where(here, pltpu.roll(v_ref[32 + t : 33 + t, :], (8 * t + 4) % LANES, 1), vown)
        vpart = jnp.where(
            here, pltpu.roll(hz_ref[64 + t : 65 + t, :], (8 * t + 4) % LANES, 1), vpart
        )
    own, part = zs_ref[pl.ds(0, KINDS), :], hz_ref[pl.ds(0, KINDS), :]
    high = lane % 8 < 4
    high1 = lane1 % 8 < 4
    top, tv = jnp.where(high, own, part), jnp.where(high1, vown, vpart)
    low, lv = jnp.where(high, part, own), jnp.where(high1, vpart, vown)

    def line(u, v):
        face = 0.5 * (v + pltpu.roll(v, LANES - 1, 1))
        f = flux(
            face, pltpu.roll(u, 1, 1), u, pltpu.roll(u, LANES - 1, 1), pltpu.roll(u, LANES - 2, 1)
        )
        return f - pltpu.roll(f, 1, 1)

    packed = jnp.where(high, line(top, tv), line(low, lv))

    def y_u(i, j):
        if j < 0:
            return lo_ref[pl.ds(((j + 2) * 4 + i) * KINDS, KINDS), :]
        if j > 3:
            return hi_ref[pl.ds(((j - 4) * 4 + i) * KINDS, KINDS), :]
        return n_ref[pl.ds((i * 4 + j) * KINDS, KINDS), :]

    def y_v(i, j):
        if j < 0:
            return lo_ref[512 + i : 513 + i, :]
        if j > 3:
            return hi_ref[512 + i : 513 + i, :]
        return v_ref[16 + i * 4 + j : 17 + i * 4 + j, :]

    def y_flux(i, j):
        face = 0.5 * (y_v(i, j) + y_v(i, j + 1))
        return flux(face, y_u(i, j - 1), y_u(i, j), y_u(i, j + 1), y_u(i, j + 2))

    for i in range(4):
        yf = y_flux(i, -1)
        for j in range(4):
            t = i * 4 + j
            up = y_flux(i, j)
            zfix = jnp.where(edge, pltpu.roll(packed, (LANES - (8 * t + 4)) % LANES, 1), 0.0)
            out_ref[pl.ds(t, KINDS, stride=TILES), :] = acc_ref[t] - 0.25 * ((up - yf) + zfix)
            yf = up


def hbm(*shape):
    return jax.ShapeDtypeStruct(shape, F32)


def vm(*shape, dtype=F32):
    return pltpu.VMEM(shape, dtype)


VM = pl.BlockSpec(memory_space=pltpu.VMEM)
SM = pl.BlockSpec(memory_space=pltpu.SMEM)


def near(x):
    return pltpu.with_memory_space_constraint(x, pltpu.VMEM)


def call(kernel, out_shape, scalars, inputs, scratch=()):
    return pl.pallas_call(
        kernel,
        out_shape=out_shape,
        in_specs=[SM] * len(scalars) + [VM] * len(inputs),
        out_specs=jax.tree.map(lambda _: VM, out_shape),
        scratch_shapes=scratch,
        compiler_params=pltpu.CompilerParams(vmem_limit_bytes=16 * 1024 * 1024),
    )(*scalars, *inputs)


def shards(
    number_densities, kinetic_kelvin, flow_vector, opacity_area, illumination,
    arrhenius_coefficient, arrhenius_barrier, exothermic_energy, emission_loss,
    participant_indices, demanding_patches,
):
    n = number_densities.reshape(KINDS * TILES, LANES)
    v = flow_vector.reshape(3 * TILES, LANES)
    temp = kinetic_kelvin.reshape(TILES, LANES)
    n2, ty, xown, zown = call(
        totals_kernel,
        (vm(TILES, KINDS, LANES), vm(256, LANES), vm(256, LANES), vm(KINDS, LANES)),
        [], [n],
    )

    size = lax.axis_size("gy")
    around = lambda count, by: [(a, (a + by) % count) for a in range(count)]

    rounds = [
        ("round_x", (1, 2, 1), lambda a: a ^ 1),
        ("round_y0", (2, 2, 1), lambda a: a ^ 2),
        ("round_y1", (2, 4, 2), lambda a: (a // 8) * 8 + (3 - (a // 2) % 4) * 2 + a % 2),
        ("round_z0", (8, 2, 1), lambda a: a ^ 8),
        ("round_z1", None, lambda a: (3 - a // 8) * 8 + a % 8),
    ]
    below, total = None, ty
    for name, later, to in rounds:
        last = lax.ppermute(total, "gy", [(a, to(a)) for a in range(size)])
        if name == "round_x":
            xpay = near(lax.ppermute(xown, "gx", around(lax.axis_size("gx"), 1)))
            zpay = near(lax.ppermute(zown, "gz", around(lax.axis_size("gz"), 1)))
        last = near(last)
        if later is not None:
            below, total = call(
                functools.partial(combine_kernel, *later),
                (vm(256, LANES), vm(256, LANES)),
                [], [last, total] + ([] if below is None else [below]),
            )

    big = (TILES, PHOTON, LANES)
    mid = (TILES, KINDS, LANES)
    (ost, g2, pg, lt, lp, cb, made, lost, heat, den, na, yl, yu, zc) = call(
        local_kernel,
        (
            vm(128, 192, dtype=BF16), vm(384, 128, dtype=BF16), vm(80, 512, dtype=BF16),
            vm(64, 512, dtype=BF16), vm(64, 256, dtype=BF16), vm(320, LANES),
            vm(*mid), vm(*mid), vm(TILES, LANES), vm(TILES, LANES), vm(*big), vm(*big),
            vm(*big), vm(TILES * KINDS, LANES),
        ),
        [illumination],
        [
            n2, temp, opacity_area.T, participant_indices, exothermic_energy[None],
            arrhenius_coefficient[None], arrhenius_barrier[None], emission_loss[None],
        ],
    )
    pe = call(
        early_kernel, vm(*big), [illumination],
        [n2, zc, xown, xpay, zown, zpay, ost],
    )
    n_new, temp_new, up, dn, zs = call(
        chemistry_kernel,
        (vm(1040, LANES), hbm(TILES, LANES), vm(520, LANES), vm(520, LANES), vm(80, LANES)),
        [demanding_patches.reshape(MAXD)],
        [
            n2, temp, v, ty, below, total, last, pe, ost, g2, pg, lt, lp, cb,
            made, lost, heat, den, na, yl, yu,
        ],
        [
            pltpu.VMEM(big, F32), pltpu.VMEM(mid, F32),
            pltpu.VMEM((MAXD, KINDS, LANES), F32), pltpu.VMEM((8, LANES), F32),
        ],
    )

    low = near(lax.ppermute(up, "gy", around(size, 1)))
    high = near(lax.ppermute(dn, "gy", around(size, -1)))
    hx = near(lax.ppermute(n_new, "gx", around(lax.axis_size("gx"), 1)))
    hz = near(lax.ppermute(zs, "gz", around(lax.axis_size("gz"), 1)))
    acc = call(inner_kernel, vm(*mid), [], [n_new, v, hx])
    out = call(
        outer_kernel, hbm(KINDS * TILES, LANES), [],
        [n_new, acc, v, low, high, zs, hz],
    )
    return out.reshape(KINDS, 4, 4, LANES), temp_new.reshape(4, 4, LANES)


def solution(mesh):
    field = P(None, "gx", "gy", "gz")
    return jax.shard_map(
        shards,
        mesh=mesh,
        in_specs=(field, P("gx", "gy", "gz"), field) + (P(),) * 7 + (P("gx", "gy", "gz", None),),
        out_specs=(field, P("gx", "gy", "gz")),
        check_vma=False,
    )
```

```python
import jax
import jax.numpy as jnp
from jax import lax
from jax.experimental import pallas as pl
from jax.experimental.pallas import tpu as pltpu
from jax.sharding import PartitionSpec as P


KINDS = 64
PHOTON = 128
NSUB = 8
TILES = 16
LANES = 128
MAXD = 4
LOG2E = 1.4426950408889634

F32 = jnp.float32
BF16 = jnp.bfloat16


def split(x):
    hi = x.astype(BF16)
    lo = (x - hi.astype(F32)).astype(BF16)
    return hi, lo


def dot(a, b):
    return jnp.dot(a, b, preferred_element_type=F32)


def totals_kernel(n_ref, n2_ref, ty_ref, xpay_ref, zpay_ref):
    tiles = []
    for t in range(TILES):
        a = n_ref[pl.ds(t, KINDS, stride=TILES), :]
        n2_ref[t] = a
        tiles.append(a)
    for q in range(4):
        ty_ref[pl.ds(q * KINDS, KINDS), :] = (tiles[4 * q] + tiles[4 * q + 1]) + (
            tiles[4 * q + 2] + tiles[4 * q + 3]
        )
        xpay_ref[pl.ds(q * KINDS, KINDS), :] = (tiles[q] + tiles[q + 4]) + (
            tiles[q + 8] + tiles[q + 12]
        )
    lane = lax.broadcasted_iota(jnp.int32, (KINDS, LANES), 1)
    tz = jnp.zeros((KINDS, LANES), F32)
    for t in range(TILES):
        tz = jnp.where(lane == t, jnp.sum(tiles[t], axis=1, keepdims=True), tz)
    zpay_ref[...] = tz


def later(block, count, least):
    here = lax.rem(lax.div(lax.axis_index("gy"), block), count)
    return jnp.where(here >= least, 1.0, 0.0).astype(F32)


def pair_kernel(own_ref, other_ref, pair_ref):
    pair_ref[...] = own_ref[...] + other_ref[...]


def plane_kernel(other_ref, pair_ref, flip_ref, turn_ref, both_ref, below_ref, plane_ref):
    flip = flip_ref[...]
    far = turn_ref[...] + both_ref[...]
    plane_ref[...] = (pair_ref[...] + flip) + far
    below_ref[...] = later(1, 2, 1) * other_ref[...] + (
        later(2, 2, 1) * flip + later(2, 4, 2) * far
    )


def stacked(x):
    hi, lo = split(x)
    return jnp.concatenate([hi, lo, hi], axis=0)


def local_kernel(
    light_ref, n2_ref, temp_ref, opt_ref, idx_ref, exo_ref, coef_ref, bar_ref, em_ref,
    ost_ref, g2_ref, pg_ref, lt_ref, lp_ref, cb_ref,
    made_ref, lost_ref, heat_ref, den_ref, na_ref, yl_ref, yu_ref, zc_ref,
):
    op_hi, op_lo = split(opt_ref[...])
    op_hi, op_lo = op_hi.astype(F32), op_lo.astype(F32)
    ost = jnp.concatenate([op_hi, op_hi, op_lo], axis=0).T.astype(BF16)
    ost_ref[...] = ost
    a, b = idx_ref[0:1, :], idx_ref[1:2, :]
    c, e = idx_ref[2:3, :], idx_ref[3:4, :]
    taken = wide([a, b[:, PHOTON:]])
    species = lax.broadcasted_iota(jnp.int32, (LANES, 384), 0) % KINDS
    hot = jnp.where(species == taken, 1.0, 0.0).astype(F32)
    g2 = jnp.concatenate([hot[:, q * 128 : (q + 1) * 128].T for q in range(3)], axis=0)
    g2 = g2.astype(BF16)
    g2_ref[...] = g2
    rows = lax.broadcasted_iota(jnp.int32, (80, 256), 0)
    made = jnp.where(rows == c, 1.0, 0.0) + jnp.where(rows == e, 1.0, 0.0)
    exo_hi, exo_lo = split(exo_ref[...])
    made = jnp.where(rows == 64, exo_hi.astype(F32), made)
    made = jnp.where(rows == 65, exo_lo.astype(F32), made)
    pg = wide([made, made]).astype(BF16)
    pg_ref[...] = pg
    rows = lax.broadcasted_iota(jnp.int32, (KINDS, 256), 0)
    lt = jnp.where(rows == wide([a[:, PHOTON:], b[:, PHOTON:]]), 1.0, 0.0)
    lt = wide([lt, lt]).astype(BF16)
    lt_ref[...] = lt
    lp = jnp.where(rows[:, :PHOTON] == a[:, :PHOTON], 1.0, 0.0)
    lp_ref[...] = wide([lp, lp]).astype(BF16)
    coef = jnp.broadcast_to(coef_ref[...], (LANES, LANES)).T
    bar = jnp.broadcast_to(bar_ref[...] * (-LOG2E), (LANES, LANES)).T
    em = jnp.broadcast_to(em_ref[...], (LANES, KINDS)).T
    cb_ref[pl.ds(0, LANES), :] = coef
    cb_ref[pl.ds(LANES, LANES), :] = bar
    cb_ref[pl.ds(2 * LANES, KINDS), :] = em
    k_in = lax.broadcasted_iota(jnp.int32, (2 * LANES, LANES), 0) % LANES
    k_out = lax.broadcasted_iota(jnp.int32, (2 * LANES, LANES), 1)
    uu = jnp.where(k_in < k_out, 1.0, jnp.where(k_in == k_out, 0.5, 0.0)).astype(BF16)
    coef, bar, em = wide([coef, coef]), wide([bar, bar]), wide([em, em])
    pgt = wide([pg[:, 128:256], pg[:, 384:512]])

    def four(i, carry):
        base = i * 4
        blk = n2_ref[pl.ds(base, 4)].reshape(256, LANES)
        zc_ref[pl.ds(i * 256, 256), :] = dot(wide(split(blk)), uu)
        tiles = [n2_ref[base + j] for j in range(4)]
        total = (tiles[0] + tiles[1]) + (tiles[2] + tiles[3])
        run = jnp.zeros_like(total)
        for p in range(2):
            a = base + 2 * p
            cols = []
            for j in (2 * p, 2 * p + 1):
                low = run + 0.5 * tiles[j]
                run = run + tiles[j]
                cols += [low, total - low]
            tau = dot(ost, stacked(wide(cols)))
            for q in range(4):
                part = light_ref[2 + q % 2] * jnp.exp2(
                    tau[:, q * 128 : (q + 1) * 128] * (-LOG2E / 128.0)
                )
                (yl_ref, yu_ref)[q % 2][a + q // 2] = part
            n = wide([tiles[2 * p], tiles[2 * p + 1]])
            temp = wide([temp_ref[pl.ds(a, 1), :], temp_ref[pl.ds(a + 1, 1), :]])
            gat = dot(g2, jnp.concatenate(split(n), axis=0))
            th = coef * jnp.exp2(bar * (1.0 / temp))
            kb = th * gat[256:384]
            ka = th * gat[128:256]
            made = dot(pgt, jnp.concatenate(split(kb * gat[128:256]), axis=0))
            lost = 1.0 + dot(
                lt, jnp.concatenate(split(jnp.concatenate([kb, ka], axis=0)), axis=0)
            )
            heat = made[64:65] + made[65:66]
            den = 1.0 + jnp.sum(em * n, axis=0, keepdims=True)
            for q in range(2):
                cut = slice(q * LANES, (q + 1) * LANES)
                made_ref[a + q] = made[:64, cut]
                lost_ref[a + q] = lost[:, cut]
                na_ref[a + q] = gat[:128, cut]
                heat_ref[pl.ds(a + q, 1), :] = heat[:, cut]
                den_ref[pl.ds(a + q, 1), :] = den[:, cut]
        return carry

    lax.fori_loop(0, 4, four, 0)


def wide(parts):
    return jnp.concatenate(parts, axis=1)


def early_kernel(light_ref, listed_ref, n2_ref, zc_ref, xown_ref, xpay_ref, zown_ref, zpay_ref, ost_ref, pe_ref):
    gx = lax.axis_index("gx").astype(F32)
    gz = lax.axis_index("gz").astype(F32)
    ost = ost_ref[...]
    zsum = zown_ref[pl.ds(0, KINDS), :] + zpay_ref[pl.ds(0, KINDS), :]
    zlow = gz * zpay_ref[pl.ds(0, KINDS), :]
    runx = [gx * xpay_ref[pl.ds(q * KINDS, KINDS), :] for q in range(4)]
    for i in range(4):
        for j in range(4):
            t = i * 4 + j
            n = n2_ref[t]
            xl = runx[j] + 0.5 * n
            runx[j] = runx[j] + n
            zl = zc_ref[pl.ds(t * KINDS, KINDS), :] + zlow[:, t : t + 1]
            xsum = xown_ref[pl.ds(j * KINDS, KINDS), :] + xpay_ref[pl.ds(j * KINDS, KINDS), :]
            tau = dot(ost, stacked(wide([xl, xsum - xl, zl, zsum[:, t : t + 1] - zl])))
            ph = None
            for q in range(4):
                size, d = ((8.0, 0), (8.0, 1), (256.0, 4), (256.0, 5))[q]
                part = light_ref[d] * jnp.exp2(tau[:, q * 128 : (q + 1) * 128] * (-LOG2E / size))
                ph = part if q == 0 else ph + part
            pe_ref[t] = ph


def chemistry_kernel(
    listed_ref,
    n2_ref, temp_ref, v_ref, ty_ref, below_ref, plane_ref, flip_ref, turn_ref, both_ref, pe_ref,
    ost_ref, g2_ref, pg_ref, lt_ref, lp_ref, cb_ref,
    made_ref, lost_ref, heat_ref, den_ref, na_ref, yl_ref, yu_ref,
    n_out, temp_out, up_out, dn_out, z_out,
    ph_ref, ll_ref, cur_ref, curt_ref,
):
    near_z, far_z = later(8, 2, 1), later(8, 4, 2)
    ost = ost_ref[...]
    for i in range(4):
        cut = pl.ds(i * KINDS, KINDS)
        flip = flip_ref[cut, :]
        away = turn_ref[cut, :] + both_ref[cut, :]
        below = below_ref[cut, :] + (near_z * flip + far_z * away)
        above = ((plane_ref[cut, :] + flip) + away) - below - ty_ref[cut, :]
        far = jnp.exp2(dot(ost, stacked(wide([below, above]))) * (-LOG2E / 128.0))
        for j in range(4):
            t = i * 4 + j
            ph_ref[t] = pe_ref[t] + (yl_ref[t] * far[:, :LANES] + yu_ref[t] * far[:, LANES:])

    lp = lp_ref[...]
    pgp = wide([pg_ref[:, 0:128], pg_ref[:, 256:384]])

    def quiet(c, carry):
        base = c * 4
        for p in range(2):
            a = base + 2 * p
            ph = wide([ph_ref[a], ph_ref[a + 1]])
            ll = dot(lp, jnp.concatenate(split(ph), axis=0))
            na = wide([na_ref[a], na_ref[a + 1]])
            made = dot(pgp, jnp.concatenate(split(ph * na), axis=0))
            heat = made[64:65] + made[65:66]
            for q in range(2):
                cut = slice(q * LANES, (q + 1) * LANES)
                ll_ref[a + q] = ll[:, cut]
                n_out[pl.ds(pl.multiple_of((a + q) * KINDS, KINDS), KINDS), :] = (n2_ref[a + q] + (made_ref[a + q] + made[:64, cut])) / (
                    lost_ref[a + q] + ll[:, cut]
                )
                row = pl.ds(a + q, 1)
                temp_out[row, :] = (temp_ref[row, :] + (heat_ref[row, :] + heat[:, cut])) / (
                    den_ref[row, :]
                )
        return carry

    lax.fori_loop(0, 4, quiet, 0)

    pick = [jnp.minimum(listed_ref[m], TILES - 1) for m in range(MAXD)]
    for m in range(MAXD):
        cur_ref[m] = n2_ref[pick[m]]
        curt_ref[pl.ds(m, 1), :] = temp_ref[pl.ds(pick[m], 1), :]
    g2, pg, lt = g2_ref[...], pg_ref[...], lt_ref[...]
    coef = cb_ref[pl.ds(0, LANES), :]
    bar = cb_ref[pl.ds(LANES, LANES), :]
    em = cb_ref[pl.ds(2 * LANES, KINDS), :]
    coef, bar, em = wide([coef, coef]), wide([bar, bar]), wide([em, em])
    h = 1.0 / NSUB

    def substep(s, carry):
        for p in range(2):
            a, b = 2 * p, 2 * p + 1
            n = wide([cur_ref[a], cur_ref[b]])
            temp = wide([curt_ref[a : a + 1, :], curt_ref[b : b + 1, :]])
            ph = wide([ph_ref[pick[a]], ph_ref[pick[b]]])
            ll = wide([ll_ref[pick[a]], ll_ref[pick[b]]])
            th = coef * jnp.exp2(bar * (1.0 / temp))
            gat = dot(g2, jnp.concatenate(split(n), axis=0))
            kb = th * gat[256:384]
            ka = th * gat[128:256]
            rate = jnp.concatenate([ph * gat[:128], kb * gat[128:256]], axis=0)
            rem = jnp.concatenate([kb, ka], axis=0)
            made = dot(pg, jnp.concatenate(split(rate), axis=0))
            lost = dot(lt, jnp.concatenate(split(rem), axis=0)) + ll
            heat = made[64:65] + made[65:66]
            cool = jnp.sum(em * n, axis=0, keepdims=True)
            nn = (n + h * made[:64]) / (1.0 + h * lost)
            tt = (temp + h * heat) / (1.0 + h * cool)
            cur_ref[a] = nn[:, :LANES]
            cur_ref[b] = nn[:, LANES:]
            curt_ref[a : a + 1, :] = tt[:, :LANES]
            curt_ref[b : b + 1, :] = tt[:, LANES:]
        return carry

    lax.fori_loop(0, NSUB, substep, 0)

    for m in range(MAXD):

        @pl.when(listed_ref[m] < TILES)
        def _():
            n_out[pl.ds(pl.multiple_of(pick[m] * KINDS, KINDS), KINDS), :] = cur_ref[m]
            temp_out[pl.ds(pick[m], 1), :] = curt_ref[m : m + 1, :]

    lane = lax.broadcasted_iota(jnp.int32, (KINDS, LANES), 1)
    zp = jnp.zeros((KINDS, LANES), F32)
    up_out[pl.ds(512, 8), :] = jnp.zeros((8, LANES), F32)
    dn_out[pl.ds(512, 8), :] = jnp.zeros((8, LANES), F32)
    for i in range(4):
        for j in range(4):
            t = i * 4 + j
            u = n_out[pl.ds(t * KINDS, KINDS), :]
            zp = jnp.where(lane // 8 == t, pltpu.roll(u, (8 * t + 4) % LANES, 1), zp)
            if j < 2:
                dn_out[pl.ds((j * 4 + i) * KINDS, KINDS), :] = u
            else:
                up_out[pl.ds(((j - 2) * 4 + i) * KINDS, KINDS), :] = u
        up_out[pl.ds(512 + i, 1), :] = v_ref[pl.ds(TILES + i * 4 + 3, 1), :]
        dn_out[pl.ds(512 + i, 1), :] = v_ref[pl.ds(TILES + i * 4, 1), :]
    z_out[pl.ds(0, KINDS), :] = zp
    n_out[pl.ds(1024, TILES), :] = v_ref[pl.ds(0, TILES), :]
    z_out[pl.ds(KINDS, TILES), :] = v_ref[pl.ds(2 * TILES, TILES), :]


def flux(face, um1, u, up1, up2):
    state = jnp.where(face > 0, 1.5 * u - 0.5 * um1, 1.5 * up1 - 0.5 * up2)
    return face * state


def inner_kernel(n_ref, v_ref, hx_ref, acc_ref):
    lane = lax.broadcasted_iota(jnp.int32, (KINDS, LANES), 1)
    edge = jnp.logical_or(lane < 2, lane >= LANES - 2)

    def x_u(i, j):
        if 0 <= i < 4:
            return n_ref[pl.ds((i * 4 + j) * KINDS, KINDS), :]
        return hx_ref[pl.ds(((i % 4) * 4 + j) * KINDS, KINDS), :]

    def x_v(i, j):
        if 0 <= i < 4:
            return v_ref[i * 4 + j : i * 4 + j + 1, :]
        r = 1024 + (i % 4) * 4 + j
        return hx_ref[r : r + 1, :]

    def x_flux(i, j):
        face = 0.5 * (x_v(i, j) + x_v(i + 1, j))
        return flux(face, x_u(i - 1, j), x_u(i, j), x_u(i + 1, j), x_u(i + 2, j))

    xf = [x_flux(-1, j) for j in range(4)]
    for i in range(4):
        for j in range(4):
            t = i * 4 + j
            u = n_ref[pl.ds(t * KINDS, KINDS), :]
            top = x_flux(i, j)
            change = top - xf[j]
            xf[j] = top
            vz = v_ref[32 + t : 33 + t, :]
            face = 0.5 * (vz + pltpu.roll(vz, LANES - 1, 1))
            fz = flux(
                face,
                pltpu.roll(u, 1, 1),
                u,
                pltpu.roll(u, LANES - 1, 1),
                pltpu.roll(u, LANES - 2, 1),
            )
            change = change + jnp.where(edge, 0.0, fz - pltpu.roll(fz, 1, 1))
            acc_ref[t] = u - 0.25 * change


def outer_kernel(n_ref, acc_ref, v_ref, lo_ref, hi_ref, zs_ref, hz_ref, out_ref):
    lane = lax.broadcasted_iota(jnp.int32, (KINDS, LANES), 1)
    lane1 = lax.broadcasted_iota(jnp.int32, (1, LANES), 1)
    edge = jnp.logical_or(lane < 2, lane >= LANES - 2)

    vown = jnp.zeros((1, LANES), F32)
    vpart = jnp.zeros((1, LANES), F32)
    for t in range(TILES):
        here = lane1 // 8 == t
        vown = jnp.where(here, pltpu.roll(v_ref[32 + t : 33 + t, :], (8 * t + 4) % LANES, 1), vown)
        vpart = jnp.where(
            here, pltpu.roll(hz_ref[64 + t : 65 + t, :], (8 * t + 4) % LANES, 1), vpart
        )
    own, part = zs_ref[pl.ds(0, KINDS), :], hz_ref[pl.ds(0, KINDS), :]
    high = lane % 8 < 4
    high1 = lane1 % 8 < 4
    top, tv = jnp.where(high, own, part), jnp.where(high1, vown, vpart)
    low, lv = jnp.where(high, part, own), jnp.where(high1, vpart, vown)

    def line(u, v):
        face = 0.5 * (v + pltpu.roll(v, LANES - 1, 1))
        f = flux(
            face, pltpu.roll(u, 1, 1), u, pltpu.roll(u, LANES - 1, 1), pltpu.roll(u, LANES - 2, 1)
        )
        return f - pltpu.roll(f, 1, 1)

    packed = jnp.where(high, line(top, tv), line(low, lv))

    def y_u(i, j):
        if j < 0:
            return lo_ref[pl.ds(((j + 2) * 4 + i) * KINDS, KINDS), :]
        if j > 3:
            return hi_ref[pl.ds(((j - 4) * 4 + i) * KINDS, KINDS), :]
        return n_ref[pl.ds((i * 4 + j) * KINDS, KINDS), :]

    def y_v(i, j):
        if j < 0:
            return lo_ref[512 + i : 513 + i, :]
        if j > 3:
            return hi_ref[512 + i : 513 + i, :]
        return v_ref[16 + i * 4 + j : 17 + i * 4 + j, :]

    def y_flux(i, j):
        face = 0.5 * (y_v(i, j) + y_v(i, j + 1))
        return flux(face, y_u(i, j - 1), y_u(i, j), y_u(i, j + 1), y_u(i, j + 2))

    for i in range(4):
        yf = y_flux(i, -1)
        for j in range(4):
            t = i * 4 + j
            up = y_flux(i, j)
            zfix = jnp.where(edge, pltpu.roll(packed, (LANES - (8 * t + 4)) % LANES, 1), 0.0)
            out_ref[pl.ds(t, KINDS, stride=TILES), :] = acc_ref[t] - 0.25 * ((up - yf) + zfix)
            yf = up


def hbm(*shape):
    return jax.ShapeDtypeStruct(shape, F32)


def vm(*shape, dtype=F32):
    return pltpu.VMEM(shape, dtype)


VM = pl.BlockSpec(memory_space=pltpu.VMEM)
SM = pl.BlockSpec(memory_space=pltpu.SMEM)


def near(x):
    return pltpu.with_memory_space_constraint(x, pltpu.VMEM)


def call(kernel, out_shape, scalars, inputs, scratch=()):
    return pl.pallas_call(
        kernel,
        out_shape=out_shape,
        in_specs=[SM] * len(scalars) + [VM] * len(inputs),
        out_specs=jax.tree.map(lambda _: VM, out_shape),
        scratch_shapes=scratch,
        compiler_params=pltpu.CompilerParams(vmem_limit_bytes=16 * 1024 * 1024),
    )(*scalars, *inputs)


def shards(
    number_densities, kinetic_kelvin, flow_vector, opacity_area, illumination,
    arrhenius_coefficient, arrhenius_barrier, exothermic_energy, emission_loss,
    participant_indices, demanding_patches,
):
    n = number_densities.reshape(KINDS * TILES, LANES)
    v = flow_vector.reshape(3 * TILES, LANES)
    temp = kinetic_kelvin.reshape(TILES, LANES)
    listed = demanding_patches.reshape(MAXD)
    n2, ty, xown, zown = call(
        totals_kernel,
        (vm(TILES, KINDS, LANES), vm(256, LANES), vm(256, LANES), vm(KINDS, LANES)),
        [], [n],
    )

    size = lax.axis_size("gy")
    around = lambda count, by: [(a, (a + by) % count) for a in range(count)]

    def send(value, to):
        return near(lax.ppermute(value, "gy", [(a, to(a)) for a in range(size)]))

    flip_y = lambda a: a ^ 2
    turn_y = lambda a: (a // 8) * 8 + (3 - (a // 2) % 4) * 2 + a % 2
    flip_z = lambda a: a ^ 8
    turn_z = lambda a: (3 - a // 8) * 8 + a % 8
    other = send(ty, lambda a: a ^ 1)
    xpay = near(lax.ppermute(xown, "gx", around(lax.axis_size("gx"), 1)))
    zpay = near(lax.ppermute(zown, "gz", around(lax.axis_size("gz"), 1)))
    pair = call(pair_kernel, vm(256, LANES), [], [ty, other])
    y_parts = [send(pair, flip_y), send(pair, turn_y), send(pair, lambda a: turn_y(flip_y(a)))]
    below, plane = call(plane_kernel, (vm(256, LANES), vm(256, LANES)), [], [other, pair] + y_parts)
    z_parts = [send(plane, flip_z), send(plane, turn_z), send(plane, lambda a: turn_z(flip_z(a)))]

    big = (TILES, PHOTON, LANES)
    mid = (TILES, KINDS, LANES)
    (ost, g2, pg, lt, lp, cb, made, lost, heat, den, na, yl, yu, zc) = call(
        local_kernel,
        (
            vm(128, 192, dtype=BF16), vm(384, 128, dtype=BF16), vm(80, 512, dtype=BF16),
            vm(64, 512, dtype=BF16), vm(64, 256, dtype=BF16), vm(320, LANES),
            vm(*mid), vm(*mid), vm(TILES, LANES), vm(TILES, LANES), vm(*big), vm(*big),
            vm(*big), vm(TILES * KINDS, LANES),
        ),
        [illumination],
        [
            n2, temp, opacity_area.T, participant_indices, exothermic_energy[None],
            arrhenius_coefficient[None], arrhenius_barrier[None], emission_loss[None],
        ],
    )
    pe = call(
        early_kernel, vm(*big), [illumination, listed],
        [n2, zc, xown, xpay, zown, zpay, ost],
    )
    n_new, temp_new, up, dn, zs = call(
        chemistry_kernel,
        (vm(1040, LANES), hbm(TILES, LANES), vm(520, LANES), vm(520, LANES), vm(80, LANES)),
        [listed],
        [
            n2, temp, v, ty, below, plane, *z_parts, pe, ost, g2, pg, lt, lp, cb,
            made, lost, heat, den, na, yl, yu,
        ],
        [
            pltpu.VMEM(big, F32), pltpu.VMEM(mid, F32),
            pltpu.VMEM((MAXD, KINDS, LANES), F32), pltpu.VMEM((8, LANES), F32),
        ],
    )

    low = near(lax.ppermute(up, "gy", around(size, 1)))
    high = near(lax.ppermute(dn, "gy", around(size, -1)))
    hx = near(lax.ppermute(n_new, "gx", around(lax.axis_size("gx"), 1)))
    hz = near(lax.ppermute(zs, "gz", around(lax.axis_size("gz"), 1)))
    acc = call(inner_kernel, vm(*mid), [], [n_new, v, hx])
    out = call(
        outer_kernel, hbm(KINDS * TILES, LANES), [],
        [n_new, acc, v, low, high, zs, hz],
    )
    return out.reshape(KINDS, 4, 4, LANES), temp_new.reshape(4, 4, LANES)


def solution(mesh):
    field = P(None, "gx", "gy", "gz")
    return jax.shard_map(
        shards,
        mesh=mesh,
        in_specs=(field, P("gx", "gy", "gz"), field) + (P(),) * 7 + (P("gx", "gy", "gz", None),),
        out_specs=(field, P("gx", "gy", "gz")),
        check_vma=False,
    )
```

```python
import jax
import jax.numpy as jnp
from jax import lax
from jax.experimental import pallas as pl
from jax.experimental.pallas import tpu as pltpu
from jax.sharding import PartitionSpec as P


KINDS = 64
PHOTON = 128
NSUB = 8
TILES = 16
LANES = 128
MAXD = 4
LOG2E = 1.4426950408889634

F32 = jnp.float32
BF16 = jnp.bfloat16


def split(x):
    hi = x.astype(BF16)
    lo = (x - hi.astype(F32)).astype(BF16)
    return hi, lo


def dot(a, b):
    return jnp.dot(a, b, preferred_element_type=F32)


def totals_kernel(n_ref, n2_ref, ty_ref, xpay_ref, zpay_ref):
    tiles = []
    for t in range(TILES):
        a = n_ref[pl.ds(t, KINDS, stride=TILES), :]
        n2_ref[t] = a
        tiles.append(a)
    for q in range(4):
        ty_ref[pl.ds(q * KINDS, KINDS), :] = (tiles[4 * q] + tiles[4 * q + 1]) + (
            tiles[4 * q + 2] + tiles[4 * q + 3]
        )
        xpay_ref[pl.ds(q * KINDS, KINDS), :] = (tiles[q] + tiles[q + 4]) + (
            tiles[q + 8] + tiles[q + 12]
        )
    lane = lax.broadcasted_iota(jnp.int32, (KINDS, LANES), 1)
    tz = jnp.zeros((KINDS, LANES), F32)
    for t in range(TILES):
        tz = jnp.where(lane == t, jnp.sum(tiles[t], axis=1, keepdims=True), tz)
    zpay_ref[...] = tz


def later(block, count, least):
    here = lax.rem(lax.div(lax.axis_index("gy"), block), count)
    return jnp.where(here >= least, 1.0, 0.0).astype(F32)


def pair_kernel(own_ref, other_ref, pair_ref):
    pair_ref[...] = own_ref[...] + other_ref[...]


def plane_kernel(other_ref, pair_ref, flip_ref, turn_ref, both_ref, below_ref, plane_ref):
    flip = flip_ref[...]
    far = turn_ref[...] + both_ref[...]
    plane_ref[...] = (pair_ref[...] + flip) + far
    below_ref[...] = later(1, 2, 1) * other_ref[...] + (
        later(2, 2, 1) * flip + later(2, 4, 2) * far
    )


def stacked(x):
    hi, lo = split(x)
    return jnp.concatenate([hi, lo, hi], axis=0)


def local_kernel(
    light_ref, n2_ref, temp_ref, opt_ref, idx_ref, exo_ref, coef_ref, bar_ref, em_ref,
    ost_ref, g2_ref, pg_ref, cb_ref,
    made_ref, lost_ref, heat_ref, den_ref, na_ref, yl_ref, yu_ref, zc_ref,
):
    op_hi, op_lo = split(opt_ref[...])
    op_hi, op_lo = op_hi.astype(F32), op_lo.astype(F32)
    ost = jnp.concatenate([op_hi, op_hi, op_lo], axis=0).T.astype(BF16)
    ost_ref[...] = ost
    a, b = idx_ref[0:1, :], idx_ref[1:2, :]
    c, e = idx_ref[2:3, :], idx_ref[3:4, :]
    taken = wide([a, b[:, PHOTON:]])
    species = lax.broadcasted_iota(jnp.int32, (LANES, 384), 0) % KINDS
    hot = jnp.where(species == taken, 1.0, 0.0).astype(F32)
    g2 = jnp.concatenate([hot[:, q * 128 : (q + 1) * 128].T for q in range(3)], axis=0)
    g2 = g2.astype(BF16)
    g2_ref[...] = g2
    rows = lax.broadcasted_iota(jnp.int32, (144, 256), 0)
    lanes = lax.broadcasted_iota(jnp.int32, (144, 256), 1)
    made = jnp.where(rows == c, 1.0, 0.0) + jnp.where(rows == e, 1.0, 0.0)
    made = made + jnp.where(rows - 80 == a, 1.0, 0.0)
    made = made + jnp.where(jnp.logical_and(rows - 80 == b, lanes >= PHOTON), 1.0, 0.0)
    exo_hi, exo_lo = split(exo_ref[...])
    made = jnp.where(rows == 64, exo_hi.astype(F32), made)
    made = jnp.where(rows == 65, exo_lo.astype(F32), made)
    pg = wide([made, made]).astype(BF16)
    pg_ref[...] = pg
    rows = lax.broadcasted_iota(jnp.int32, (KINDS, 256), 0)
    lt = jnp.where(rows == wide([a[:, PHOTON:], b[:, PHOTON:]]), 1.0, 0.0)
    lt = wide([lt, lt]).astype(BF16)
    coef = jnp.broadcast_to(coef_ref[...], (LANES, LANES)).T
    bar = jnp.broadcast_to(bar_ref[...] * (-LOG2E), (LANES, LANES)).T
    em = jnp.broadcast_to(em_ref[...], (LANES, KINDS)).T
    cb_ref[pl.ds(0, LANES), :] = coef
    cb_ref[pl.ds(LANES, LANES), :] = bar
    cb_ref[pl.ds(2 * LANES, KINDS), :] = em
    k_in = lax.broadcasted_iota(jnp.int32, (2 * LANES, LANES), 0) % LANES
    k_out = lax.broadcasted_iota(jnp.int32, (2 * LANES, LANES), 1)
    uu = jnp.where(k_in < k_out, 1.0, jnp.where(k_in == k_out, 0.5, 0.0)).astype(BF16)
    coef, bar, em = wide([coef, coef]), wide([bar, bar]), wide([em, em])
    pgt = wide([pg[:80, 128:256], pg[:80, 384:512]])

    def four(i, carry):
        base = i * 4
        blk = n2_ref[pl.ds(base, 4)].reshape(256, LANES)
        zc_ref[pl.ds(i * 256, 256), :] = dot(wide(split(blk)), uu)
        tiles = [n2_ref[base + j] for j in range(4)]
        total = (tiles[0] + tiles[1]) + (tiles[2] + tiles[3])
        run = jnp.zeros_like(total)
        for p in range(2):
            a = base + 2 * p
            cols = []
            for j in (2 * p, 2 * p + 1):
                low = run + 0.5 * tiles[j]
                run = run + tiles[j]
                cols += [low, total - low]
            tau = dot(ost, stacked(wide(cols)))
            for q in range(4):
                part = light_ref[2 + q % 2] * jnp.exp2(
                    tau[:, q * 128 : (q + 1) * 128] * (-LOG2E / 128.0)
                )
                (yl_ref, yu_ref)[q % 2][a + q // 2] = part
            n = wide([tiles[2 * p], tiles[2 * p + 1]])
            temp = wide([temp_ref[pl.ds(a, 1), :], temp_ref[pl.ds(a + 1, 1), :]])
            gat = dot(g2, jnp.concatenate(split(n), axis=0))
            th = coef * jnp.exp2(bar * (1.0 / temp))
            kb = th * gat[256:384]
            ka = th * gat[128:256]
            made = dot(pgt, jnp.concatenate(split(kb * gat[128:256]), axis=0))
            lost = 1.0 + dot(
                lt, jnp.concatenate(split(jnp.concatenate([kb, ka], axis=0)), axis=0)
            )
            heat = made[64:65] + made[65:66]
            den = 1.0 + jnp.sum(em * n, axis=0, keepdims=True)
            for q in range(2):
                cut = slice(q * LANES, (q + 1) * LANES)
                made_ref[a + q] = made[:64, cut]
                lost_ref[a + q] = lost[:, cut]
                na_ref[a + q] = gat[:128, cut]
                heat_ref[pl.ds(a + q, 1), :] = heat[:, cut]
                den_ref[pl.ds(a + q, 1), :] = den[:, cut]
        return carry

    lax.fori_loop(0, 4, four, 0)


def wide(parts):
    return jnp.concatenate(parts, axis=1)


def early_kernel(light_ref, listed_ref, n2_ref, zc_ref, xown_ref, xpay_ref, zown_ref, zpay_ref, ost_ref, pe_ref, list_out):
    gx = lax.axis_index("gx").astype(F32)
    gz = lax.axis_index("gz").astype(F32)
    for m in range(MAXD):
        list_out[m : m + 1, :] = jnp.full((1, LANES), listed_ref[m], jnp.int32)
    ost = ost_ref[...]
    zsum = zown_ref[pl.ds(0, KINDS), :] + zpay_ref[pl.ds(0, KINDS), :]
    zlow = gz * zpay_ref[pl.ds(0, KINDS), :]
    runx = [gx * xpay_ref[pl.ds(q * KINDS, KINDS), :] for q in range(4)]
    for i in range(4):
        for j in range(4):
            t = i * 4 + j
            n = n2_ref[t]
            xl = runx[j] + 0.5 * n
            runx[j] = runx[j] + n
            zl = zc_ref[pl.ds(t * KINDS, KINDS), :] + zlow[:, t : t + 1]
            xsum = xown_ref[pl.ds(j * KINDS, KINDS), :] + xpay_ref[pl.ds(j * KINDS, KINDS), :]
            tau = dot(ost, stacked(wide([xl, xsum - xl, zl, zsum[:, t : t + 1] - zl])))
            ph = None
            for q in range(4):
                size, d = ((8.0, 0), (8.0, 1), (256.0, 4), (256.0, 5))[q]
                part = light_ref[d] * jnp.exp2(tau[:, q * 128 : (q + 1) * 128] * (-LOG2E / size))
                ph = part if q == 0 else ph + part
            pe_ref[t] = ph


def chemistry_kernel(
    listed_ref,
    n2_ref, temp_ref, v_ref, ty_ref, below_ref, plane_ref, flip_ref, turn_ref, both_ref, pe_ref,
    ost_ref, g2_ref, pg_ref, cb_ref,
    made_ref, lost_ref, heat_ref, den_ref, na_ref, yl_ref, yu_ref,
    n_out, temp_out, up_out, dn_out, z_out,
    ph_ref, cur_ref, curt_ref,
):
    near_z, far_z = later(8, 2, 1), later(8, 4, 2)
    ost = ost_ref[...]
    for i in range(4):
        cut = pl.ds(i * KINDS, KINDS)
        flip = flip_ref[cut, :]
        away = turn_ref[cut, :] + both_ref[cut, :]
        below = below_ref[cut, :] + (near_z * flip + far_z * away)
        above = ((plane_ref[cut, :] + flip) + away) - below - ty_ref[cut, :]
        far = jnp.exp2(dot(ost, stacked(wide([below, above]))) * (-LOG2E / 128.0))
        for j in range(4):
            t = i * 4 + j
            ph_ref[t] = pe_ref[t] + (yl_ref[t] * far[:, :LANES] + yu_ref[t] * far[:, LANES:])

    pgp = wide([pg_ref[:, 0:128], pg_ref[:, 256:384]])

    def quiet(c, carry):
        base = c * 4
        for p in range(2):
            a = base + 2 * p
            ph = wide([ph_ref[a], ph_ref[a + 1]])
            na = wide([na_ref[a], na_ref[a + 1]])
            made = dot(pgp, jnp.concatenate(split(ph * na), axis=0))
            heat = made[64:65] + made[65:66]
            for q in range(2):
                cut = slice(q * LANES, (q + 1) * LANES)
                n = n2_ref[a + q]
                n_out[pl.ds(pl.multiple_of((a + q) * KINDS, KINDS), KINDS), :] = (
                    n * (n + (made_ref[a + q] + made[:64, cut]))
                ) / (lost_ref[a + q] * n + made[80:, cut])
                row = pl.ds(a + q, 1)
                temp_out[row, :] = (temp_ref[row, :] + (heat_ref[row, :] + heat[:, cut])) / (
                    den_ref[row, :]
                )
        return carry

    lax.fori_loop(0, 4, quiet, 0)

    listed = [listed_ref[m, 0] for m in range(MAXD)]
    pick = [jnp.minimum(listed[m], TILES - 1) for m in range(MAXD)]
    for m in range(MAXD):
        cur_ref[m] = n2_ref[pick[m]]
        curt_ref[pl.ds(m, 1), :] = temp_ref[pl.ds(pick[m], 1), :]
    g2, pg = g2_ref[...], pg_ref[...]
    coef = cb_ref[pl.ds(0, LANES), :]
    bar = cb_ref[pl.ds(LANES, LANES), :]
    em = cb_ref[pl.ds(2 * LANES, KINDS), :]
    coef, bar, em = wide([coef, coef]), wide([bar, bar]), wide([em, em])
    h = 1.0 / NSUB

    def substep(s, carry):
        for p in range(2):
            a, b = 2 * p, 2 * p + 1
            n = wide([cur_ref[a], cur_ref[b]])
            temp = wide([curt_ref[a : a + 1, :], curt_ref[b : b + 1, :]])
            ph = wide([ph_ref[pick[a]], ph_ref[pick[b]]])
            th = coef * jnp.exp2(bar * (1.0 / temp))
            gat = dot(g2, jnp.concatenate(split(n), axis=0))
            rate = jnp.concatenate(
                [ph * gat[:128], th * gat[128:256] * gat[256:384]], axis=0
            )
            made = dot(pg, jnp.concatenate(split(rate), axis=0))
            heat = made[64:65] + made[65:66]
            cool = jnp.sum(em * n, axis=0, keepdims=True)
            nn = (n * (n + h * made[:64])) / (n + h * made[80:])
            tt = (temp + h * heat) / (1.0 + h * cool)
            cur_ref[a] = nn[:, :LANES]
            cur_ref[b] = nn[:, LANES:]
            curt_ref[a : a + 1, :] = tt[:, :LANES]
            curt_ref[b : b + 1, :] = tt[:, LANES:]
        return carry

    lax.fori_loop(0, NSUB, substep, 0)

    for m in range(MAXD):

        @pl.when(listed[m] < TILES)
        def _():
            n_out[pl.ds(pl.multiple_of(pick[m] * KINDS, KINDS), KINDS), :] = cur_ref[m]
            temp_out[pl.ds(pick[m], 1), :] = curt_ref[m : m + 1, :]

    lane = lax.broadcasted_iota(jnp.int32, (KINDS, LANES), 1)
    zp = jnp.zeros((KINDS, LANES), F32)
    up_out[pl.ds(512, 8), :] = jnp.zeros((8, LANES), F32)
    dn_out[pl.ds(512, 8), :] = jnp.zeros((8, LANES), F32)
    for i in range(4):
        for j in range(4):
            t = i * 4 + j
            u = n_out[pl.ds(t * KINDS, KINDS), :]
            zp = jnp.where(lane // 8 == t, pltpu.roll(u, (8 * t + 4) % LANES, 1), zp)
            if j < 2:
                dn_out[pl.ds((j * 4 + i) * KINDS, KINDS), :] = u
            else:
                up_out[pl.ds(((j - 2) * 4 + i) * KINDS, KINDS), :] = u
        up_out[pl.ds(512 + i, 1), :] = v_ref[pl.ds(TILES + i * 4 + 3, 1), :]
        dn_out[pl.ds(512 + i, 1), :] = v_ref[pl.ds(TILES + i * 4, 1), :]
    z_out[pl.ds(0, KINDS), :] = zp
    n_out[pl.ds(1024, TILES), :] = v_ref[pl.ds(0, TILES), :]
    z_out[pl.ds(KINDS, TILES), :] = v_ref[pl.ds(2 * TILES, TILES), :]


def flux(face, um1, u, up1, up2):
    state = jnp.where(face > 0, 1.5 * u - 0.5 * um1, 1.5 * up1 - 0.5 * up2)
    return face * state


def inner_kernel(n_ref, v_ref, hx_ref, acc_ref):
    lane = lax.broadcasted_iota(jnp.int32, (KINDS, LANES), 1)
    edge = jnp.logical_or(lane < 2, lane >= LANES - 2)

    def x_u(i, j):
        if 0 <= i < 4:
            return n_ref[pl.ds((i * 4 + j) * KINDS, KINDS), :]
        return hx_ref[pl.ds(((i % 4) * 4 + j) * KINDS, KINDS), :]

    def x_v(i, j):
        if 0 <= i < 4:
            return v_ref[i * 4 + j : i * 4 + j + 1, :]
        r = 1024 + (i % 4) * 4 + j
        return hx_ref[r : r + 1, :]

    def x_flux(i, j):
        face = 0.5 * (x_v(i, j) + x_v(i + 1, j))
        return flux(face, x_u(i - 1, j), x_u(i, j), x_u(i + 1, j), x_u(i + 2, j))

    xf = [x_flux(-1, j) for j in range(4)]
    for i in range(4):
        for j in range(4):
            t = i * 4 + j
            u = n_ref[pl.ds(t * KINDS, KINDS), :]
            top = x_flux(i, j)
            change = top - xf[j]
            xf[j] = top
            vz = v_ref[32 + t : 33 + t, :]
            face = 0.5 * (vz + pltpu.roll(vz, LANES - 1, 1))
            fz = flux(
                face,
                pltpu.roll(u, 1, 1),
                u,
                pltpu.roll(u, LANES - 1, 1),
                pltpu.roll(u, LANES - 2, 1),
            )
            change = change + jnp.where(edge, 0.0, fz - pltpu.roll(fz, 1, 1))
            acc_ref[t] = u - 0.25 * change


def outer_kernel(n_ref, acc_ref, v_ref, lo_ref, hi_ref, zs_ref, hz_ref, out_ref):
    lane = lax.broadcasted_iota(jnp.int32, (KINDS, LANES), 1)
    lane1 = lax.broadcasted_iota(jnp.int32, (1, LANES), 1)
    edge = jnp.logical_or(lane < 2, lane >= LANES - 2)

    vown = jnp.zeros((1, LANES), F32)
    vpart = jnp.zeros((1, LANES), F32)
    for t in range(TILES):
        here = lane1 // 8 == t
        vown = jnp.where(here, pltpu.roll(v_ref[32 + t : 33 + t, :], (8 * t + 4) % LANES, 1), vown)
        vpart = jnp.where(
            here, pltpu.roll(hz_ref[64 + t : 65 + t, :], (8 * t + 4) % LANES, 1), vpart
        )
    own, part = zs_ref[pl.ds(0, KINDS), :], hz_ref[pl.ds(0, KINDS), :]
    high = lane % 8 < 4
    high1 = lane1 % 8 < 4
    top, tv = jnp.where(high, own, part), jnp.where(high1, vown, vpart)
    low, lv = jnp.where(high, part, own), jnp.where(high1, vpart, vown)

    def line(u, v):
        face = 0.5 * (v + pltpu.roll(v, LANES - 1, 1))
        f = flux(
            face, pltpu.roll(u, 1, 1), u, pltpu.roll(u, LANES - 1, 1), pltpu.roll(u, LANES - 2, 1)
        )
        return f - pltpu.roll(f, 1, 1)

    packed = jnp.where(high, line(top, tv), line(low, lv))

    def y_u(i, j):
        if j < 0:
            return lo_ref[pl.ds(((j + 2) * 4 + i) * KINDS, KINDS), :]
        if j > 3:
            return hi_ref[pl.ds(((j - 4) * 4 + i) * KINDS, KINDS), :]
        return n_ref[pl.ds((i * 4 + j) * KINDS, KINDS), :]

    def y_v(i, j):
        if j < 0:
            return lo_ref[512 + i : 513 + i, :]
        if j > 3:
            return hi_ref[512 + i : 513 + i, :]
        return v_ref[16 + i * 4 + j : 17 + i * 4 + j, :]

    def y_flux(i, j):
        face = 0.5 * (y_v(i, j) + y_v(i, j + 1))
        return flux(face, y_u(i, j - 1), y_u(i, j), y_u(i, j + 1), y_u(i, j + 2))

    for i in range(4):
        yf = y_flux(i, -1)
        for j in range(4):
            t = i * 4 + j
            up = y_flux(i, j)
            zfix = jnp.where(edge, pltpu.roll(packed, (LANES - (8 * t + 4)) % LANES, 1), 0.0)
            out_ref[pl.ds(t, KINDS, stride=TILES), :] = acc_ref[t] - 0.25 * ((up - yf) + zfix)
            yf = up


def hbm(*shape):
    return jax.ShapeDtypeStruct(shape, F32)


def vm(*shape, dtype=F32):
    return pltpu.VMEM(shape, dtype)


VM = pl.BlockSpec(memory_space=pltpu.VMEM)
SM = pl.BlockSpec(memory_space=pltpu.SMEM)


def near(x):
    return pltpu.with_memory_space_constraint(x, pltpu.VMEM)


def call(kernel, out_shape, scalars, inputs, scratch=()):
    return pl.pallas_call(
        kernel,
        out_shape=out_shape,
        in_specs=[SM] * len(scalars) + [VM] * len(inputs),
        out_specs=jax.tree.map(lambda _: VM, out_shape),
        scratch_shapes=scratch,
        compiler_params=pltpu.CompilerParams(vmem_limit_bytes=16 * 1024 * 1024),
    )(*scalars, *inputs)


def shards(
    number_densities, kinetic_kelvin, flow_vector, opacity_area, illumination,
    arrhenius_coefficient, arrhenius_barrier, exothermic_energy, emission_loss,
    participant_indices, demanding_patches,
):
    n = number_densities.reshape(KINDS * TILES, LANES)
    v = flow_vector.reshape(3 * TILES, LANES)
    temp = kinetic_kelvin.reshape(TILES, LANES)
    listed = demanding_patches.reshape(MAXD)
    n2, ty, xown, zown = call(
        totals_kernel,
        (vm(TILES, KINDS, LANES), vm(256, LANES), vm(256, LANES), vm(KINDS, LANES)),
        [], [n],
    )

    size = lax.axis_size("gy")
    around = lambda count, by: [(a, (a + by) % count) for a in range(count)]

    def send(value, to):
        return near(lax.ppermute(value, "gy", [(a, to(a)) for a in range(size)]))

    flip_y = lambda a: a ^ 2
    turn_y = lambda a: (a // 8) * 8 + (3 - (a // 2) % 4) * 2 + a % 2
    flip_z = lambda a: a ^ 8
    turn_z = lambda a: (3 - a // 8) * 8 + a % 8
    other = send(ty, lambda a: a ^ 1)
    xpay = near(lax.ppermute(xown, "gx", around(lax.axis_size("gx"), 1)))
    zpay = near(lax.ppermute(zown, "gz", around(lax.axis_size("gz"), 1)))
    pair = call(pair_kernel, vm(256, LANES), [], [ty, other])
    y_parts = [send(pair, flip_y), send(pair, turn_y), send(pair, lambda a: turn_y(flip_y(a)))]
    below, plane = call(plane_kernel, (vm(256, LANES), vm(256, LANES)), [], [other, pair] + y_parts)
    z_parts = [send(plane, flip_z), send(plane, turn_z), send(plane, lambda a: turn_z(flip_z(a)))]

    big = (TILES, PHOTON, LANES)
    mid = (TILES, KINDS, LANES)
    (ost, g2, pg, cb, made, lost, heat, den, na, yl, yu, zc) = call(
        local_kernel,
        (
            vm(128, 192, dtype=BF16), vm(384, 128, dtype=BF16), vm(144, 512, dtype=BF16),
            vm(320, LANES),
            vm(*mid), vm(*mid), vm(TILES, LANES), vm(TILES, LANES), vm(*big), vm(*big),
            vm(*big), vm(TILES * KINDS, LANES),
        ),
        [illumination],
        [
            n2, temp, opacity_area.T, participant_indices, exothermic_energy[None],
            arrhenius_coefficient[None], arrhenius_barrier[None], emission_loss[None],
        ],
    )
    pe, tiles = call(
        early_kernel, (vm(*big), vm(8, LANES, dtype=jnp.int32)), [illumination, listed],
        [n2, zc, xown, xpay, zown, zpay, ost],
    )
    n_new, temp_new, up, dn, zs = call(
        chemistry_kernel,
        (vm(1040, LANES), vm(TILES, LANES), vm(520, LANES), vm(520, LANES), vm(80, LANES)),
        [],
        [
            tiles, n2, temp, v, ty, below, plane, *z_parts, pe, ost, g2, pg, cb,
            made, lost, heat, den, na, yl, yu,
        ],
        [
            pltpu.VMEM(big, F32),
            pltpu.VMEM((MAXD, KINDS, LANES), F32), pltpu.VMEM((8, LANES), F32),
        ],
    )

    low = near(lax.ppermute(up, "gy", around(size, 1)))
    high = near(lax.ppermute(dn, "gy", around(size, -1)))
    hx = near(lax.ppermute(n_new, "gx", around(lax.axis_size("gx"), 1)))
    hz = near(lax.ppermute(zs, "gz", around(lax.axis_size("gz"), 1)))
    acc = call(inner_kernel, vm(*mid), [], [n_new, v, hx])
    out = call(
        outer_kernel, hbm(KINDS * TILES, LANES), [],
        [n_new, acc, v, low, high, zs, hz],
    )
    return out.reshape(KINDS, 4, 4, LANES), temp_new.reshape(4, 4, LANES)


def solution(mesh):
    field = P(None, "gx", "gy", "gz")
    return jax.shard_map(
        shards,
        mesh=mesh,
        in_specs=(field, P("gx", "gy", "gz"), field) + (P(),) * 7 + (P("gx", "gy", "gz", None),),
        out_specs=(field, P("gx", "gy", "gz")),
        check_vma=False,
    )
```

```python
import jax
import jax.numpy as jnp
from jax import lax
from jax.experimental import pallas as pl
from jax.experimental.pallas import tpu as pltpu
from jax.sharding import PartitionSpec as P


KINDS = 64
PHOTON = 128
NSUB = 8
TILES = 16
LANES = 128
MAXD = 4
LOG2E = 1.4426950408889634

F32 = jnp.float32
BF16 = jnp.bfloat16


def split(x):
    hi = x.astype(BF16)
    lo = (x - hi.astype(F32)).astype(BF16)
    return hi, lo


def dot(a, b):
    return jnp.dot(a, b, preferred_element_type=F32)


def totals_kernel(n_ref, n2_ref, ty_ref, xpay_ref, zpay_ref):
    tiles = []
    for t in range(TILES):
        a = n_ref[pl.ds(t, KINDS, stride=TILES), :]
        n2_ref[t] = a
        tiles.append(a)
    for q in range(4):
        ty_ref[pl.ds(q * KINDS, KINDS), :] = (tiles[4 * q] + tiles[4 * q + 1]) + (
            tiles[4 * q + 2] + tiles[4 * q + 3]
        )
        xpay_ref[pl.ds(q * KINDS, KINDS), :] = (tiles[q] + tiles[q + 4]) + (
            tiles[q + 8] + tiles[q + 12]
        )
    lane = lax.broadcasted_iota(jnp.int32, (KINDS, LANES), 1)
    tz = jnp.zeros((KINDS, LANES), F32)
    for t in range(TILES):
        tz = jnp.where(lane == t, jnp.sum(tiles[t], axis=1, keepdims=True), tz)
    zpay_ref[...] = tz


def later(block, count, least):
    here = lax.rem(lax.div(lax.axis_index("gy"), block), count)
    return jnp.where(here >= least, 1.0, 0.0).astype(F32)


def pair_kernel(own_ref, other_ref, pair_ref):
    pair_ref[...] = own_ref[...] + other_ref[...]


def plane_kernel(other_ref, pair_ref, flip_ref, turn_ref, both_ref, below_ref, plane_ref):
    flip = flip_ref[...]
    far = turn_ref[...] + both_ref[...]
    plane_ref[...] = (pair_ref[...] + flip) + far
    below_ref[...] = later(1, 2, 1) * other_ref[...] + (
        later(2, 2, 1) * flip + later(2, 4, 2) * far
    )


def stacked(x):
    hi, lo = split(x)
    return jnp.concatenate([hi, lo, hi], axis=0)


def local_kernel(
    light_ref, n2_ref, temp_ref, opt_ref, idx_ref, exo_ref, coef_ref, bar_ref, em_ref,
    ost_ref, g2_ref, pg_ref, cb_ref,
    made_ref, lost_ref, heat_ref, den_ref, na_ref, yl_ref, yu_ref, zc_ref,
):
    op_hi, op_lo = split(opt_ref[...])
    op_hi, op_lo = op_hi.astype(F32), op_lo.astype(F32)
    ost = jnp.concatenate([op_hi, op_hi, op_lo], axis=0).T.astype(BF16)
    ost_ref[...] = ost
    a, b = idx_ref[0:1, :], idx_ref[1:2, :]
    c, e = idx_ref[2:3, :], idx_ref[3:4, :]
    taken = wide([a, b[:, PHOTON:]])
    species = lax.broadcasted_iota(jnp.int32, (LANES, 384), 0) % KINDS
    hot = jnp.where(species == taken, 1.0, 0.0).astype(F32)
    g2 = jnp.concatenate([hot[:, q * 128 : (q + 1) * 128].T for q in range(3)], axis=0)
    g2 = g2.astype(BF16)
    g2_ref[...] = g2
    rows = lax.broadcasted_iota(jnp.int32, (144, 256), 0)
    lanes = lax.broadcasted_iota(jnp.int32, (144, 256), 1)
    made = jnp.where(rows == c, 1.0, 0.0) + jnp.where(rows == e, 1.0, 0.0)
    made = made + jnp.where(rows - 80 == a, 1.0, 0.0)
    made = made + jnp.where(jnp.logical_and(rows - 80 == b, lanes >= PHOTON), 1.0, 0.0)
    exo_hi, exo_lo = split(exo_ref[...])
    made = jnp.where(rows == 64, exo_hi.astype(F32), made)
    made = jnp.where(rows == 65, exo_lo.astype(F32), made)
    pg = wide([made, made]).astype(BF16)
    pg_ref[...] = pg
    rows = lax.broadcasted_iota(jnp.int32, (KINDS, 256), 0)
    lt = jnp.where(rows == wide([a[:, PHOTON:], b[:, PHOTON:]]), 1.0, 0.0)
    lt = wide([lt, lt]).astype(BF16)
    coef = jnp.broadcast_to(coef_ref[...], (LANES, LANES)).T
    bar = jnp.broadcast_to(bar_ref[...] * (-LOG2E), (LANES, LANES)).T
    em = jnp.broadcast_to(em_ref[...], (LANES, KINDS)).T
    cb_ref[pl.ds(0, LANES), :] = coef
    cb_ref[pl.ds(LANES, LANES), :] = bar
    cb_ref[pl.ds(2 * LANES, KINDS), :] = em
    k_in = lax.broadcasted_iota(jnp.int32, (2 * LANES, LANES), 0) % LANES
    k_out = lax.broadcasted_iota(jnp.int32, (2 * LANES, LANES), 1)
    uu = jnp.where(k_in < k_out, 1.0, jnp.where(k_in == k_out, 0.5, 0.0)).astype(BF16)
    coef, bar, em = wide([coef, coef]), wide([bar, bar]), wide([em, em])
    pgt = wide([pg[:80, 128:256], pg[:80, 384:512]])

    def four(i, carry):
        base = i * 4
        blk = n2_ref[pl.ds(base, 4)].reshape(256, LANES)
        zc_ref[pl.ds(i * 256, 256), :] = dot(wide(split(blk)), uu)
        tiles = [n2_ref[base + j] for j in range(4)]
        total = (tiles[0] + tiles[1]) + (tiles[2] + tiles[3])
        run = jnp.zeros_like(total)
        for p in range(2):
            a = base + 2 * p
            cols = []
            for j in (2 * p, 2 * p + 1):
                low = run + 0.5 * tiles[j]
                run = run + tiles[j]
                cols += [low, total - low]
            tau = dot(ost, stacked(wide(cols)))
            for q in range(4):
                part = light_ref[2 + q % 2] * jnp.exp2(
                    tau[:, q * 128 : (q + 1) * 128] * (-LOG2E / 128.0)
                )
                (yl_ref, yu_ref)[q % 2][a + q // 2] = part
            n = wide([tiles[2 * p], tiles[2 * p + 1]])
            temp = wide([temp_ref[pl.ds(a, 1), :], temp_ref[pl.ds(a + 1, 1), :]])
            gat = dot(g2, jnp.concatenate(split(n), axis=0))
            th = coef * jnp.exp2(bar * (1.0 / temp))
            kb = th * gat[256:384]
            ka = th * gat[128:256]
            made = dot(pgt, jnp.concatenate(split(kb * gat[128:256]), axis=0))
            lost = 1.0 + dot(
                lt, jnp.concatenate(split(jnp.concatenate([kb, ka], axis=0)), axis=0)
            )
            heat = made[64:65] + made[65:66]
            den = 1.0 + jnp.sum(em * n, axis=0, keepdims=True)
            for q in range(2):
                cut = slice(q * LANES, (q + 1) * LANES)
                made_ref[a + q] = made[:64, cut]
                lost_ref[a + q] = lost[:, cut]
                na_ref[a + q] = gat[:128, cut]
                heat_ref[pl.ds(a + q, 1), :] = heat[:, cut]
                den_ref[pl.ds(a + q, 1), :] = den[:, cut]
        return carry

    lax.fori_loop(0, 4, four, 0)


def wide(parts):
    return jnp.concatenate(parts, axis=1)


def early_kernel(light_ref, listed_ref, n2_ref, zc_ref, xown_ref, xpay_ref, zown_ref, zpay_ref, ost_ref, pe_ref, list_out):
    gx = lax.axis_index("gx").astype(F32)
    gz = lax.axis_index("gz").astype(F32)
    for m in range(MAXD):
        list_out[m : m + 1, :] = jnp.full((1, LANES), listed_ref[m], jnp.int32)
    ost = ost_ref[...]
    zsum = zown_ref[pl.ds(0, KINDS), :] + zpay_ref[pl.ds(0, KINDS), :]
    zlow = gz * zpay_ref[pl.ds(0, KINDS), :]
    runx = [gx * xpay_ref[pl.ds(q * KINDS, KINDS), :] for q in range(4)]
    for i in range(4):
        for j in range(4):
            t = i * 4 + j
            n = n2_ref[t]
            xl = runx[j] + 0.5 * n
            runx[j] = runx[j] + n
            zl = zc_ref[pl.ds(t * KINDS, KINDS), :] + zlow[:, t : t + 1]
            xsum = xown_ref[pl.ds(j * KINDS, KINDS), :] + xpay_ref[pl.ds(j * KINDS, KINDS), :]
            tau = dot(ost, stacked(wide([xl, xsum - xl, zl, zsum[:, t : t + 1] - zl])))
            ph = None
            for q in range(4):
                size, d = ((8.0, 0), (8.0, 1), (256.0, 4), (256.0, 5))[q]
                part = light_ref[d] * jnp.exp2(tau[:, q * 128 : (q + 1) * 128] * (-LOG2E / size))
                ph = part if q == 0 else ph + part
            pe_ref[t] = ph


def chemistry_kernel(
    listed_ref,
    n2_ref, temp_ref, v_ref, ty_ref, below_ref, plane_ref, flip_ref, turn_ref, both_ref, pe_ref,
    ost_ref, g2_ref, pg_ref, cb_ref,
    made_ref, lost_ref, heat_ref, den_ref, na_ref, yl_ref, yu_ref,
    n_out, temp_out, up_out, dn_out, z_out,
    ph_ref, cur_ref, curt_ref,
):
    near_z, far_z = later(8, 2, 1), later(8, 4, 2)
    ost = ost_ref[...]
    for i in range(4):
        cut = pl.ds(i * KINDS, KINDS)
        flip = flip_ref[cut, :]
        away = turn_ref[cut, :] + both_ref[cut, :]
        below = below_ref[cut, :] + (near_z * flip + far_z * away)
        above = ((plane_ref[cut, :] + flip) + away) - below - ty_ref[cut, :]
        far = jnp.exp2(dot(ost, stacked(wide([below, above]))) * (-LOG2E / 128.0))
        for j in range(4):
            t = i * 4 + j
            ph_ref[t] = pe_ref[t] + (yl_ref[t] * far[:, :LANES] + yu_ref[t] * far[:, LANES:])

    pgp = wide([pg_ref[:, 0:128], pg_ref[:, 256:384]])

    def quiet(c, carry):
        base = c * 4
        for p in range(2):
            a = base + 2 * p
            ph = wide([ph_ref[a], ph_ref[a + 1]])
            na = wide([na_ref[a], na_ref[a + 1]])
            made = dot(pgp, jnp.concatenate(split(ph * na), axis=0))
            heat = made[64:65] + made[65:66]
            for q in range(2):
                cut = slice(q * LANES, (q + 1) * LANES)
                n = n2_ref[a + q]
                n_out[pl.ds(pl.multiple_of((a + q) * KINDS, KINDS), KINDS), :] = (
                    n * (n + (made_ref[a + q] + made[:64, cut]))
                ) / (lost_ref[a + q] * n + made[80:, cut])
                row = pl.ds(a + q, 1)
                temp_out[row, :] = (temp_ref[row, :] + (heat_ref[row, :] + heat[:, cut])) / (
                    den_ref[row, :]
                )
        return carry

    lax.fori_loop(0, 4, quiet, 0)

    listed = [listed_ref[m, 0] for m in range(MAXD)]
    pick = [jnp.minimum(listed[m], TILES - 1) for m in range(MAXD)]
    for m in range(MAXD):
        cur_ref[m] = n2_ref[pick[m]]
        curt_ref[pl.ds(m, 1), :] = temp_ref[pl.ds(pick[m], 1), :]
    g2, pg = g2_ref[...], pg_ref[...]
    coef = cb_ref[pl.ds(0, LANES), :]
    bar = cb_ref[pl.ds(LANES, LANES), :]
    em = cb_ref[pl.ds(2 * LANES, KINDS), :]
    coef, bar, em = wide([coef, coef]), wide([bar, bar]), wide([em, em])
    h = 1.0 / NSUB

    def substep(s, carry):
        both = [(0, 1), (2, 3)]
        n = [wide([cur_ref[a], cur_ref[b]]) for a, b in both]
        temp = [wide([curt_ref[a : a + 1, :], curt_ref[b : b + 1, :]]) for a, b in both]
        ph = [wide([ph_ref[pick[a]], ph_ref[pick[b]]]) for a, b in both]
        gat = [dot(g2, jnp.concatenate(split(x), axis=0)) for x in n]
        th = [coef * jnp.exp2(bar * (1.0 / x)) for x in temp]
        light = [p * g[:128] for p, g in zip(ph, gat)]
        dark = [t * g[128:256] * g[256:384] for t, g in zip(th, gat)]
        made = [
            dot(pg, jnp.concatenate(split(jnp.concatenate(x, axis=0)), axis=0))
            for x in zip(light, dark)
        ]
        cool = [jnp.sum(em * x, axis=0, keepdims=True) for x in n]
        new_n = [(x * (x + h * m[:64])) / (x + h * m[80:]) for x, m in zip(n, made)]
        new_t = [
            (t + h * (m[64:65] + m[65:66])) / (1.0 + h * c) for t, m, c in zip(temp, made, cool)
        ]
        for q, (a, b) in enumerate(both):
            cur_ref[a] = new_n[q][:, :LANES]
            cur_ref[b] = new_n[q][:, LANES:]
            curt_ref[a : a + 1, :] = new_t[q][:, :LANES]
            curt_ref[b : b + 1, :] = new_t[q][:, LANES:]
        return carry

    lax.fori_loop(0, NSUB, substep, 0)

    for m in range(MAXD):

        @pl.when(listed[m] < TILES)
        def _():
            n_out[pl.ds(pl.multiple_of(pick[m] * KINDS, KINDS), KINDS), :] = cur_ref[m]
            temp_out[pl.ds(pick[m], 1), :] = curt_ref[m : m + 1, :]

    lane = lax.broadcasted_iota(jnp.int32, (KINDS, LANES), 1)
    zp = jnp.zeros((KINDS, LANES), F32)
    up_out[pl.ds(512, 8), :] = jnp.zeros((8, LANES), F32)
    dn_out[pl.ds(512, 8), :] = jnp.zeros((8, LANES), F32)
    for i in range(4):
        for j in range(4):
            t = i * 4 + j
            u = n_out[pl.ds(t * KINDS, KINDS), :]
            zp = jnp.where(lane // 8 == t, pltpu.roll(u, (8 * t + 4) % LANES, 1), zp)
            if j < 2:
                dn_out[pl.ds((j * 4 + i) * KINDS, KINDS), :] = u
            else:
                up_out[pl.ds(((j - 2) * 4 + i) * KINDS, KINDS), :] = u
        up_out[pl.ds(512 + i, 1), :] = v_ref[pl.ds(TILES + i * 4 + 3, 1), :]
        dn_out[pl.ds(512 + i, 1), :] = v_ref[pl.ds(TILES + i * 4, 1), :]
    z_out[pl.ds(0, KINDS), :] = zp
    n_out[pl.ds(1024, TILES), :] = v_ref[pl.ds(0, TILES), :]
    z_out[pl.ds(KINDS, TILES), :] = v_ref[pl.ds(2 * TILES, TILES), :]


def flux(face, um1, u, up1, up2):
    state = jnp.where(face > 0, 1.5 * u - 0.5 * um1, 1.5 * up1 - 0.5 * up2)
    return face * state


def inner_kernel(n_ref, v_ref, hx_ref, acc_ref):
    lane = lax.broadcasted_iota(jnp.int32, (KINDS, LANES), 1)
    edge = jnp.logical_or(lane < 2, lane >= LANES - 2)

    def x_u(i, j):
        if 0 <= i < 4:
            return n_ref[pl.ds((i * 4 + j) * KINDS, KINDS), :]
        return hx_ref[pl.ds(((i % 4) * 4 + j) * KINDS, KINDS), :]

    def x_v(i, j):
        if 0 <= i < 4:
            return v_ref[i * 4 + j : i * 4 + j + 1, :]
        r = 1024 + (i % 4) * 4 + j
        return hx_ref[r : r + 1, :]

    def x_flux(i, j):
        face = 0.5 * (x_v(i, j) + x_v(i + 1, j))
        return flux(face, x_u(i - 1, j), x_u(i, j), x_u(i + 1, j), x_u(i + 2, j))

    xf = [x_flux(-1, j) for j in range(4)]
    for i in range(4):
        for j in range(4):
            t = i * 4 + j
            u = n_ref[pl.ds(t * KINDS, KINDS), :]
            top = x_flux(i, j)
            change = top - xf[j]
            xf[j] = top
            vz = v_ref[32 + t : 33 + t, :]
            face = 0.5 * (vz + pltpu.roll(vz, LANES - 1, 1))
            fz = flux(
                face,
                pltpu.roll(u, 1, 1),
                u,
                pltpu.roll(u, LANES - 1, 1),
                pltpu.roll(u, LANES - 2, 1),
            )
            change = change + jnp.where(edge, 0.0, fz - pltpu.roll(fz, 1, 1))
            acc_ref[t] = u - 0.25 * change


def outer_kernel(n_ref, acc_ref, v_ref, lo_ref, hi_ref, zs_ref, hz_ref, out_ref):
    lane = lax.broadcasted_iota(jnp.int32, (KINDS, LANES), 1)
    lane1 = lax.broadcasted_iota(jnp.int32, (1, LANES), 1)
    edge = jnp.logical_or(lane < 2, lane >= LANES - 2)

    vown = jnp.zeros((1, LANES), F32)
    vpart = jnp.zeros((1, LANES), F32)
    for t in range(TILES):
        here = lane1 // 8 == t
        vown = jnp.where(here, pltpu.roll(v_ref[32 + t : 33 + t, :], (8 * t + 4) % LANES, 1), vown)
        vpart = jnp.where(
            here, pltpu.roll(hz_ref[64 + t : 65 + t, :], (8 * t + 4) % LANES, 1), vpart
        )
    own, part = zs_ref[pl.ds(0, KINDS), :], hz_ref[pl.ds(0, KINDS), :]
    high = lane % 8 < 4
    high1 = lane1 % 8 < 4
    top, tv = jnp.where(high, own, part), jnp.where(high1, vown, vpart)
    low, lv = jnp.where(high, part, own), jnp.where(high1, vpart, vown)

    def line(u, v):
        face = 0.5 * (v + pltpu.roll(v, LANES - 1, 1))
        f = flux(
            face, pltpu.roll(u, 1, 1), u, pltpu.roll(u, LANES - 1, 1), pltpu.roll(u, LANES - 2, 1)
        )
        return f - pltpu.roll(f, 1, 1)

    packed = jnp.where(high, line(top, tv), line(low, lv))

    def y_u(i, j):
        if j < 0:
            return lo_ref[pl.ds(((j + 2) * 4 + i) * KINDS, KINDS), :]
        if j > 3:
            return hi_ref[pl.ds(((j - 4) * 4 + i) * KINDS, KINDS), :]
        return n_ref[pl.ds((i * 4 + j) * KINDS, KINDS), :]

    def y_v(i, j):
        if j < 0:
            return lo_ref[512 + i : 513 + i, :]
        if j > 3:
            return hi_ref[512 + i : 513 + i, :]
        return v_ref[16 + i * 4 + j : 17 + i * 4 + j, :]

    def y_flux(i, j):
        face = 0.5 * (y_v(i, j) + y_v(i, j + 1))
        return flux(face, y_u(i, j - 1), y_u(i, j), y_u(i, j + 1), y_u(i, j + 2))

    for i in range(4):
        yf = y_flux(i, -1)
        for j in range(4):
            t = i * 4 + j
            up = y_flux(i, j)
            zfix = jnp.where(edge, pltpu.roll(packed, (LANES - (8 * t + 4)) % LANES, 1), 0.0)
            out_ref[pl.ds(t, KINDS, stride=TILES), :] = acc_ref[t] - 0.25 * ((up - yf) + zfix)
            yf = up


def hbm(*shape):
    return jax.ShapeDtypeStruct(shape, F32)


def vm(*shape, dtype=F32):
    return pltpu.VMEM(shape, dtype)


VM = pl.BlockSpec(memory_space=pltpu.VMEM)
SM = pl.BlockSpec(memory_space=pltpu.SMEM)


def near(x):
    return pltpu.with_memory_space_constraint(x, pltpu.VMEM)


def call(kernel, out_shape, scalars, inputs, scratch=()):
    return pl.pallas_call(
        kernel,
        out_shape=out_shape,
        in_specs=[SM] * len(scalars) + [VM] * len(inputs),
        out_specs=jax.tree.map(lambda _: VM, out_shape),
        scratch_shapes=scratch,
        compiler_params=pltpu.CompilerParams(vmem_limit_bytes=16 * 1024 * 1024),
    )(*scalars, *inputs)


def shards(
    number_densities, kinetic_kelvin, flow_vector, opacity_area, illumination,
    arrhenius_coefficient, arrhenius_barrier, exothermic_energy, emission_loss,
    participant_indices, demanding_patches,
):
    n = number_densities.reshape(KINDS * TILES, LANES)
    v = flow_vector.reshape(3 * TILES, LANES)
    temp = kinetic_kelvin.reshape(TILES, LANES)
    listed = demanding_patches.reshape(MAXD)
    n2, ty, xown, zown = call(
        totals_kernel,
        (vm(TILES, KINDS, LANES), vm(256, LANES), vm(256, LANES), vm(KINDS, LANES)),
        [], [n],
    )

    size = lax.axis_size("gy")
    around = lambda count, by: [(a, (a + by) % count) for a in range(count)]

    def send(value, to):
        return near(lax.ppermute(value, "gy", [(a, to(a)) for a in range(size)]))

    flip_y = lambda a: a ^ 2
    turn_y = lambda a: (a // 8) * 8 + (3 - (a // 2) % 4) * 2 + a % 2
    flip_z = lambda a: a ^ 8
    turn_z = lambda a: (3 - a // 8) * 8 + a % 8
    other = send(ty, lambda a: a ^ 1)
    xpay = near(lax.ppermute(xown, "gx", around(lax.axis_size("gx"), 1)))
    zpay = near(lax.ppermute(zown, "gz", around(lax.axis_size("gz"), 1)))
    pair = call(pair_kernel, vm(256, LANES), [], [ty, other])
    y_parts = [send(pair, flip_y), send(pair, turn_y), send(pair, lambda a: turn_y(flip_y(a)))]
    below, plane = call(plane_kernel, (vm(256, LANES), vm(256, LANES)), [], [other, pair] + y_parts)
    z_parts = [send(plane, flip_z), send(plane, turn_z), send(plane, lambda a: turn_z(flip_z(a)))]

    big = (TILES, PHOTON, LANES)
    mid = (TILES, KINDS, LANES)
    (ost, g2, pg, cb, made, lost, heat, den, na, yl, yu, zc) = call(
        local_kernel,
        (
            vm(128, 192, dtype=BF16), vm(384, 128, dtype=BF16), vm(144, 512, dtype=BF16),
            vm(320, LANES),
            vm(*mid), vm(*mid), vm(TILES, LANES), vm(TILES, LANES), vm(*big), vm(*big),
            vm(*big), vm(TILES * KINDS, LANES),
        ),
        [illumination],
        [
            n2, temp, opacity_area.T, participant_indices, exothermic_energy[None],
            arrhenius_coefficient[None], arrhenius_barrier[None], emission_loss[None],
        ],
    )
    pe, tiles = call(
        early_kernel, (vm(*big), vm(8, LANES, dtype=jnp.int32)), [illumination, listed],
        [n2, zc, xown, xpay, zown, zpay, ost],
    )
    n_new, temp_new, up, dn, zs = call(
        chemistry_kernel,
        (vm(1040, LANES), vm(TILES, LANES), vm(520, LANES), vm(520, LANES), vm(80, LANES)),
        [],
        [
            tiles, n2, temp, v, ty, below, plane, *z_parts, pe, ost, g2, pg, cb,
            made, lost, heat, den, na, yl, yu,
        ],
        [
            pltpu.VMEM(big, F32),
            pltpu.VMEM((MAXD, KINDS, LANES), F32), pltpu.VMEM((8, LANES), F32),
        ],
    )

    low = near(lax.ppermute(up, "gy", around(size, 1)))
    high = near(lax.ppermute(dn, "gy", around(size, -1)))
    hx = near(lax.ppermute(n_new, "gx", around(lax.axis_size("gx"), 1)))
    hz = near(lax.ppermute(zs, "gz", around(lax.axis_size("gz"), 1)))
    acc = call(inner_kernel, vm(*mid), [], [n_new, v, hx])
    out = call(
        outer_kernel, hbm(KINDS * TILES, LANES), [],
        [n_new, acc, v, low, high, zs, hz],
    )
    return out.reshape(KINDS, 4, 4, LANES), temp_new.reshape(4, 4, LANES)


def solution(mesh):
    field = P(None, "gx", "gy", "gz")
    return jax.shard_map(
        shards,
        mesh=mesh,
        in_specs=(field, P("gx", "gy", "gz"), field) + (P(),) * 7 + (P("gx", "gy", "gz", None),),
        out_specs=(field, P("gx", "gy", "gz")),
        check_vma=False,
    )
```

```python
import jax
import jax.numpy as jnp
from jax import lax
from jax.experimental import pallas as pl
from jax.experimental.pallas import tpu as pltpu
from jax.sharding import PartitionSpec as P


KINDS = 64
PHOTON = 128
NSUB = 8
TILES = 16
LANES = 128
MAXD = 4
LOG2E = 1.4426950408889634

F32 = jnp.float32
BF16 = jnp.bfloat16


def split(x):
    hi = x.astype(BF16)
    lo = (x - hi.astype(F32)).astype(BF16)
    return hi, lo


def dot(a, b):
    return jnp.dot(a, b, preferred_element_type=F32)


def totals_kernel(n_ref, n2_ref, ty_ref, xpay_ref, zpay_ref):
    tiles = []
    for t in range(TILES):
        a = n_ref[pl.ds(t, KINDS, stride=TILES), :]
        n2_ref[t] = a
        tiles.append(a)
    for q in range(4):
        ty_ref[pl.ds(q * KINDS, KINDS), :] = (tiles[4 * q] + tiles[4 * q + 1]) + (
            tiles[4 * q + 2] + tiles[4 * q + 3]
        )
        xpay_ref[pl.ds(q * KINDS, KINDS), :] = (tiles[q] + tiles[q + 4]) + (
            tiles[q + 8] + tiles[q + 12]
        )
    lane = lax.broadcasted_iota(jnp.int32, (KINDS, LANES), 1)
    tz = jnp.zeros((KINDS, LANES), F32)
    for t in range(TILES):
        tz = jnp.where(lane == t, jnp.sum(tiles[t], axis=1, keepdims=True), tz)
    zpay_ref[...] = tz


def later(block, count, least):
    here = lax.rem(lax.div(lax.axis_index("gy"), block), count)
    return jnp.where(here >= least, 1.0, 0.0).astype(F32)


def pair_kernel(own_ref, other_ref, pair_ref):
    pair_ref[...] = own_ref[...] + other_ref[...]


def plane_kernel(other_ref, pair_ref, flip_ref, turn_ref, both_ref, below_ref, plane_ref):
    flip = flip_ref[...]
    far = turn_ref[...] + both_ref[...]
    plane_ref[...] = (pair_ref[...] + flip) + far
    below_ref[...] = later(1, 2, 1) * other_ref[...] + (
        later(2, 2, 1) * flip + later(2, 4, 2) * far
    )


def stacked(x):
    hi, lo = split(x)
    return jnp.concatenate([hi, lo, hi], axis=0)


def local_kernel(
    light_ref, n2_ref, temp_ref, opt_ref, idx_ref, exo_ref, coef_ref, bar_ref, em_ref,
    ost_ref, g2_ref, pg_ref, cb_ref,
    made_ref, lost_ref, heat_ref, den_ref, na_ref, yl_ref, yu_ref, zc_ref,
):
    op_hi, op_lo = split(opt_ref[...])
    op_hi, op_lo = op_hi.astype(F32), op_lo.astype(F32)
    ost = jnp.concatenate([op_hi, op_hi, op_lo], axis=0).T.astype(BF16)
    ost_ref[...] = ost
    a, b = idx_ref[0:1, :], idx_ref[1:2, :]
    c, e = idx_ref[2:3, :], idx_ref[3:4, :]
    taken = wide([a, b[:, PHOTON:]])
    species = lax.broadcasted_iota(jnp.int32, (LANES, 384), 0) % KINDS
    hot = jnp.where(species == taken, 1.0, 0.0).astype(F32)
    g2 = jnp.concatenate([hot[:, q * 128 : (q + 1) * 128].T for q in range(3)], axis=0)
    g2 = g2.astype(BF16)
    g2_ref[...] = g2
    rows = lax.broadcasted_iota(jnp.int32, (144, 256), 0)
    lanes = lax.broadcasted_iota(jnp.int32, (144, 256), 1)
    made = jnp.where(rows == c, 1.0, 0.0) + jnp.where(rows == e, 1.0, 0.0)
    made = made + jnp.where(rows - 80 == a, 1.0, 0.0)
    made = made + jnp.where(jnp.logical_and(rows - 80 == b, lanes >= PHOTON), 1.0, 0.0)
    exo_hi, exo_lo = split(exo_ref[...])
    made = jnp.where(rows == 64, exo_hi.astype(F32), made)
    made = jnp.where(rows == 65, exo_lo.astype(F32), made)
    pg = wide([made, made]).astype(BF16)
    pg_ref[...] = pg
    rows = lax.broadcasted_iota(jnp.int32, (KINDS, 256), 0)
    lt = jnp.where(rows == wide([a[:, PHOTON:], b[:, PHOTON:]]), 1.0, 0.0)
    lt = wide([lt, lt]).astype(BF16)
    coef = jnp.broadcast_to(coef_ref[...], (LANES, LANES)).T
    bar = jnp.broadcast_to(bar_ref[...] * (-LOG2E), (LANES, LANES)).T
    em = jnp.broadcast_to(em_ref[...], (LANES, KINDS)).T
    cb_ref[pl.ds(0, LANES), :] = coef
    cb_ref[pl.ds(LANES, LANES), :] = bar
    cb_ref[pl.ds(2 * LANES, KINDS), :] = em
    k_in = lax.broadcasted_iota(jnp.int32, (2 * LANES, LANES), 0) % LANES
    k_out = lax.broadcasted_iota(jnp.int32, (2 * LANES, LANES), 1)
    uu = jnp.where(k_in < k_out, 1.0, jnp.where(k_in == k_out, 0.5, 0.0)).astype(BF16)
    coef, bar, em = wide([coef, coef]), wide([bar, bar]), wide([em, em])
    pgt = wide([pg[:80, 128:256], pg[:80, 384:512]])

    def four(i, carry):
        base = i * 4
        blk = n2_ref[pl.ds(base, 4)].reshape(256, LANES)
        zc_ref[pl.ds(i * 256, 256), :] = dot(wide(split(blk)), uu)
        tiles = [n2_ref[base + j] for j in range(4)]
        total = (tiles[0] + tiles[1]) + (tiles[2] + tiles[3])
        run = jnp.zeros_like(total)
        for p in range(2):
            a = base + 2 * p
            cols = []
            for j in (2 * p, 2 * p + 1):
                low = run + 0.5 * tiles[j]
                run = run + tiles[j]
                cols += [low, total - low]
            tau = dot(ost, stacked(wide(cols)))
            for q in range(4):
                part = light_ref[2 + q % 2] * jnp.exp2(
                    tau[:, q * 128 : (q + 1) * 128] * (-LOG2E / 128.0)
                )
                (yl_ref, yu_ref)[q % 2][a + q // 2] = part
            n = wide([tiles[2 * p], tiles[2 * p + 1]])
            temp = wide([temp_ref[pl.ds(a, 1), :], temp_ref[pl.ds(a + 1, 1), :]])
            gat = dot(g2, jnp.concatenate(split(n), axis=0))
            th = coef * jnp.exp2(bar * (1.0 / temp))
            kb = th * gat[256:384]
            ka = th * gat[128:256]
            made = dot(pgt, jnp.concatenate(split(kb * gat[128:256]), axis=0))
            lost = 1.0 + dot(
                lt, jnp.concatenate(split(jnp.concatenate([kb, ka], axis=0)), axis=0)
            )
            heat = made[64:65] + made[65:66]
            den = 1.0 + jnp.sum(em * n, axis=0, keepdims=True)
            for q in range(2):
                cut = slice(q * LANES, (q + 1) * LANES)
                made_ref[a + q] = made[:64, cut]
                lost_ref[a + q] = lost[:, cut]
                na_ref[a + q] = gat[:128, cut]
                heat_ref[pl.ds(a + q, 1), :] = heat[:, cut]
                den_ref[pl.ds(a + q, 1), :] = den[:, cut]
        return carry

    lax.fori_loop(0, 4, four, 0)


def wide(parts):
    return jnp.concatenate(parts, axis=1)


def early_kernel(light_ref, listed_ref, n2_ref, zc_ref, xown_ref, xpay_ref, zown_ref, zpay_ref, ost_ref, pe_ref, list_out):
    gx = lax.axis_index("gx").astype(F32)
    gz = lax.axis_index("gz").astype(F32)
    for m in range(MAXD):
        list_out[m : m + 1, :] = jnp.full((1, LANES), listed_ref[m], jnp.int32)
    ost = ost_ref[...]
    zsum = zown_ref[pl.ds(0, KINDS), :] + zpay_ref[pl.ds(0, KINDS), :]
    zlow = gz * zpay_ref[pl.ds(0, KINDS), :]
    runx = [gx * xpay_ref[pl.ds(q * KINDS, KINDS), :] for q in range(4)]
    for i in range(4):
        for j in range(4):
            t = i * 4 + j
            n = n2_ref[t]
            xl = runx[j] + 0.5 * n
            runx[j] = runx[j] + n
            zl = zc_ref[pl.ds(t * KINDS, KINDS), :] + zlow[:, t : t + 1]
            xsum = xown_ref[pl.ds(j * KINDS, KINDS), :] + xpay_ref[pl.ds(j * KINDS, KINDS), :]
            tau = dot(ost, stacked(wide([xl, xsum - xl, zl, zsum[:, t : t + 1] - zl])))
            ph = None
            for q in range(4):
                size, d = ((8.0, 0), (8.0, 1), (256.0, 4), (256.0, 5))[q]
                part = light_ref[d] * jnp.exp2(tau[:, q * 128 : (q + 1) * 128] * (-LOG2E / size))
                ph = part if q == 0 else ph + part
            pe_ref[t] = ph


def chemistry_kernel(
    listed_ref,
    n2_ref, temp_ref, v_ref, ty_ref, below_ref, plane_ref, flip_ref, turn_ref, both_ref, pe_ref,
    ost_ref, g2_ref, pg_ref, cb_ref,
    made_ref, lost_ref, heat_ref, den_ref, na_ref, yl_ref, yu_ref,
    up_out, temp_out, ph_ref, cur_ref, curt_ref,
):
    near_z, far_z = later(8, 2, 1), later(8, 4, 2)
    ost = ost_ref[...]
    for i in range(4):
        cut = pl.ds(i * KINDS, KINDS)
        flip = flip_ref[cut, :]
        away = turn_ref[cut, :] + both_ref[cut, :]
        below = below_ref[cut, :] + (near_z * flip + far_z * away)
        above = ((plane_ref[cut, :] + flip) + away) - below - ty_ref[cut, :]
        far = jnp.exp2(dot(ost, stacked(wide([below, above]))) * (-LOG2E / 128.0))
        for j in range(4):
            t = i * 4 + j
            ph_ref[t] = pe_ref[t] + (yl_ref[t] * far[:, :LANES] + yu_ref[t] * far[:, LANES:])

    quiet_half(2, n2_ref, temp_ref, ph_ref, pg_ref, made_ref, lost_ref, heat_ref, den_ref, na_ref, up_out, temp_out)

    listed = [listed_ref[m, 0] for m in range(MAXD)]
    pick = [jnp.minimum(listed[m], TILES - 1) for m in range(MAXD)]
    for m in range(MAXD):
        cur_ref[m] = n2_ref[pick[m]]
        curt_ref[pl.ds(m, 1), :] = temp_ref[pl.ds(pick[m], 1), :]
    g2, pg = g2_ref[...], pg_ref[...]
    coef = cb_ref[pl.ds(0, LANES), :]
    bar = cb_ref[pl.ds(LANES, LANES), :]
    em = cb_ref[pl.ds(2 * LANES, KINDS), :]
    coef, bar, em = wide([coef, coef]), wide([bar, bar]), wide([em, em])
    h = 1.0 / NSUB

    def substep(s, carry):
        both = [(0, 1), (2, 3)]
        n = [wide([cur_ref[a], cur_ref[b]]) for a, b in both]
        temp = [wide([curt_ref[a : a + 1, :], curt_ref[b : b + 1, :]]) for a, b in both]
        ph = [wide([ph_ref[pick[a]], ph_ref[pick[b]]]) for a, b in both]
        gat = [dot(g2, jnp.concatenate(split(x), axis=0)) for x in n]
        th = [coef * jnp.exp2(bar * (1.0 / x)) for x in temp]
        light = [p * g[:128] for p, g in zip(ph, gat)]
        dark = [t * g[128:256] * g[256:384] for t, g in zip(th, gat)]
        made = [
            dot(pg, jnp.concatenate(split(jnp.concatenate(x, axis=0)), axis=0))
            for x in zip(light, dark)
        ]
        cool = [jnp.sum(em * x, axis=0, keepdims=True) for x in n]
        new_n = [(x * (x + h * m[:64])) / (x + h * m[80:]) for x, m in zip(n, made)]
        new_t = [
            (t + h * (m[64:65] + m[65:66])) / (1.0 + h * c) for t, m, c in zip(temp, made, cool)
        ]
        for q, (a, b) in enumerate(both):
            cur_ref[a] = new_n[q][:, :LANES]
            cur_ref[b] = new_n[q][:, LANES:]
            curt_ref[a : a + 1, :] = new_t[q][:, :LANES]
            curt_ref[b : b + 1, :] = new_t[q][:, LANES:]
        return carry

    lax.fori_loop(0, NSUB, substep, 0, unroll=2)

    place(2, listed, cur_ref, curt_ref, up_out, temp_out)
    for i in range(4):
        up_out[pl.ds(512 + i, 1), :] = v_ref[pl.ds(TILES + i * 4 + 3, 1), :]
    velocities(2, v_ref, up_out)


def quiet_half(first, n2_ref, temp_ref, ph_ref, pg_ref, made_ref, lost_ref, heat_ref, den_ref, na_ref, out_ref, temp_out):
    pgp = wide([pg_ref[:, 0:128], pg_ref[:, 256:384]])

    def two(c, carry):
        for p in range(2):
            i = 2 * c + p
            a = i * 4 + first
            rate = wide([ph_ref[a] * na_ref[a], ph_ref[a + 1] * na_ref[a + 1]])
            made = dot(pgp, jnp.concatenate(split(rate), axis=0))
            heat = made[64:65] + made[65:66]
            for q in range(2):
                cut = slice(q * LANES, (q + 1) * LANES)
                n = n2_ref[a + q]
                out_ref[pl.ds(pl.multiple_of((q * 4 + i) * KINDS, KINDS), KINDS), :] = (
                    n * (n + (made_ref[a + q] + made[:64, cut]))
                ) / (lost_ref[a + q] * n + made[80:, cut])
                row = pl.ds(a + q, 1)
                temp_out[row, :] = (temp_ref[row, :] + (heat_ref[row, :] + heat[:, cut])) / (
                    den_ref[row, :]
                )
        return carry

    lax.fori_loop(0, 2, two, 0)


def place(first, listed, cur_ref, curt_ref, out_ref, temp_out):
    for m in range(MAXD):
        column = lax.rem(listed[m], 4)
        here = jnp.logical_and(column >= first, column < first + 2)

        @pl.when(jnp.logical_and(listed[m] < TILES, here))
        def _():
            slot = (column - first) * 4 + lax.div(listed[m], 4)
            out_ref[pl.ds(pl.multiple_of(slot * KINDS, KINDS), KINDS), :] = cur_ref[m]
            temp_out[pl.ds(listed[m], 1), :] = curt_ref[m : m + 1, :]


def velocities(first, v_ref, out_ref):
    out_ref[pl.ds(516, 4), :] = jnp.zeros((4, LANES), F32)
    for q in range(2):
        for i in range(4):
            t = i * 4 + first + q
            out_ref[pl.ds(520 + q * 4 + i, 1), :] = v_ref[pl.ds(t, 1), :]


def lower_kernel(
    listed_ref, n2_ref, temp_ref, v_ref, ph_ref, pg_ref,
    made_ref, lost_ref, heat_ref, den_ref, na_ref, cur_ref, curt_ref, up_ref, half_ref,
    temp_out, dn_out, z_out,
):
    temp_out[...] = half_ref[...]
    quiet_half(0, n2_ref, temp_ref, ph_ref, pg_ref, made_ref, lost_ref, heat_ref, den_ref, na_ref, dn_out, temp_out)
    listed = [listed_ref[m, 0] for m in range(MAXD)]
    place(0, listed, cur_ref, curt_ref, dn_out, temp_out)
    for i in range(4):
        dn_out[pl.ds(512 + i, 1), :] = v_ref[pl.ds(TILES + i * 4, 1), :]
    velocities(0, v_ref, dn_out)
    lane = lax.broadcasted_iota(jnp.int32, (KINDS, LANES), 1)
    zp = jnp.zeros((KINDS, LANES), F32)
    for i in range(4):
        for j in range(4):
            t = i * 4 + j
            u = (dn_out, up_ref)[j // 2][pl.ds((j % 2 * 4 + i) * KINDS, KINDS), :]
            zp = jnp.where(lane // 8 == t, pltpu.roll(u, (8 * t + 4) % LANES, 1), zp)
    z_out[pl.ds(0, KINDS), :] = zp
    z_out[pl.ds(KINDS, TILES), :] = v_ref[pl.ds(2 * TILES, TILES), :]


def cells(halves, i, j):
    return halves[j // 2][pl.ds((j % 2 * 4 + i) * KINDS, KINDS), :]


def flux(face, um1, u, up1, up2):
    state = jnp.where(face > 0, 1.5 * u - 0.5 * um1, 1.5 * up1 - 0.5 * up2)
    return face * state


def inner_kernel(dn_ref, up_ref, v_ref, xdn_ref, xup_ref, acc_ref):
    lane = lax.broadcasted_iota(jnp.int32, (KINDS, LANES), 1)
    edge = jnp.logical_or(lane < 2, lane >= LANES - 2)

    def x_u(i, j):
        if 0 <= i < 4:
            return cells((dn_ref, up_ref), i, j)
        return cells((xdn_ref, xup_ref), i % 4, j)

    def x_v(i, j):
        if 0 <= i < 4:
            return v_ref[i * 4 + j : i * 4 + j + 1, :]
        r = 520 + j % 2 * 4 + i % 4
        return (xdn_ref, xup_ref)[j // 2][r : r + 1, :]

    def x_flux(i, j):
        face = 0.5 * (x_v(i, j) + x_v(i + 1, j))
        return flux(face, x_u(i - 1, j), x_u(i, j), x_u(i + 1, j), x_u(i + 2, j))

    xf = [x_flux(-1, j) for j in range(4)]
    for i in range(4):
        for j in range(4):
            t = i * 4 + j
            u = cells((dn_ref, up_ref), i, j)
            top = x_flux(i, j)
            change = top - xf[j]
            xf[j] = top
            vz = v_ref[32 + t : 33 + t, :]
            face = 0.5 * (vz + pltpu.roll(vz, LANES - 1, 1))
            fz = flux(
                face,
                pltpu.roll(u, 1, 1),
                u,
                pltpu.roll(u, LANES - 1, 1),
                pltpu.roll(u, LANES - 2, 1),
            )
            change = change + jnp.where(edge, 0.0, fz - pltpu.roll(fz, 1, 1))
            acc_ref[t] = u - 0.25 * change


def outer_kernel(dn_ref, up_ref, acc_ref, v_ref, lo_ref, hi_ref, zs_ref, hz_ref, out_ref):
    lane = lax.broadcasted_iota(jnp.int32, (KINDS, LANES), 1)
    lane1 = lax.broadcasted_iota(jnp.int32, (1, LANES), 1)
    edge = jnp.logical_or(lane < 2, lane >= LANES - 2)

    vown = jnp.zeros((1, LANES), F32)
    vpart = jnp.zeros((1, LANES), F32)
    for t in range(TILES):
        here = lane1 // 8 == t
        vown = jnp.where(here, pltpu.roll(v_ref[32 + t : 33 + t, :], (8 * t + 4) % LANES, 1), vown)
        vpart = jnp.where(
            here, pltpu.roll(hz_ref[64 + t : 65 + t, :], (8 * t + 4) % LANES, 1), vpart
        )
    own, part = zs_ref[pl.ds(0, KINDS), :], hz_ref[pl.ds(0, KINDS), :]
    high = lane % 8 < 4
    high1 = lane1 % 8 < 4
    top, tv = jnp.where(high, own, part), jnp.where(high1, vown, vpart)
    low, lv = jnp.where(high, part, own), jnp.where(high1, vpart, vown)

    def line(u, v):
        face = 0.5 * (v + pltpu.roll(v, LANES - 1, 1))
        f = flux(
            face, pltpu.roll(u, 1, 1), u, pltpu.roll(u, LANES - 1, 1), pltpu.roll(u, LANES - 2, 1)
        )
        return f - pltpu.roll(f, 1, 1)

    packed = jnp.where(high, line(top, tv), line(low, lv))

    def y_u(i, j):
        if j < 0:
            return lo_ref[pl.ds(((j + 2) * 4 + i) * KINDS, KINDS), :]
        if j > 3:
            return hi_ref[pl.ds(((j - 4) * 4 + i) * KINDS, KINDS), :]
        return cells((dn_ref, up_ref), i, j)

    def y_v(i, j):
        if j < 0:
            return lo_ref[512 + i : 513 + i, :]
        if j > 3:
            return hi_ref[512 + i : 513 + i, :]
        return v_ref[16 + i * 4 + j : 17 + i * 4 + j, :]

    def y_flux(i, j):
        face = 0.5 * (y_v(i, j) + y_v(i, j + 1))
        return flux(face, y_u(i, j - 1), y_u(i, j), y_u(i, j + 1), y_u(i, j + 2))

    for i in range(4):
        yf = y_flux(i, -1)
        for j in range(4):
            t = i * 4 + j
            up = y_flux(i, j)
            zfix = jnp.where(edge, pltpu.roll(packed, (LANES - (8 * t + 4)) % LANES, 1), 0.0)
            out_ref[pl.ds(t, KINDS, stride=TILES), :] = acc_ref[t] - 0.25 * ((up - yf) + zfix)
            yf = up


def hbm(*shape):
    return jax.ShapeDtypeStruct(shape, F32)


def vm(*shape, dtype=F32):
    return pltpu.VMEM(shape, dtype)


VM = pl.BlockSpec(memory_space=pltpu.VMEM)
SM = pl.BlockSpec(memory_space=pltpu.SMEM)


def near(x):
    return pltpu.with_memory_space_constraint(x, pltpu.VMEM)


def call(kernel, out_shape, scalars, inputs, scratch=()):
    return pl.pallas_call(
        kernel,
        out_shape=out_shape,
        in_specs=[SM] * len(scalars) + [VM] * len(inputs),
        out_specs=jax.tree.map(lambda _: VM, out_shape),
        scratch_shapes=scratch,
        compiler_params=pltpu.CompilerParams(vmem_limit_bytes=16 * 1024 * 1024),
    )(*scalars, *inputs)


def shards(
    number_densities, kinetic_kelvin, flow_vector, opacity_area, illumination,
    arrhenius_coefficient, arrhenius_barrier, exothermic_energy, emission_loss,
    participant_indices, demanding_patches,
):
    n = number_densities.reshape(KINDS * TILES, LANES)
    v = flow_vector.reshape(3 * TILES, LANES)
    temp = kinetic_kelvin.reshape(TILES, LANES)
    listed = demanding_patches.reshape(MAXD)
    n2, ty, xown, zown = call(
        totals_kernel,
        (vm(TILES, KINDS, LANES), vm(256, LANES), vm(256, LANES), vm(KINDS, LANES)),
        [], [n],
    )

    size = lax.axis_size("gy")
    around = lambda count, by: [(a, (a + by) % count) for a in range(count)]

    def send(value, to):
        return near(lax.ppermute(value, "gy", [(a, to(a)) for a in range(size)]))

    flip_y = lambda a: a ^ 2
    turn_y = lambda a: (a // 8) * 8 + (3 - (a // 2) % 4) * 2 + a % 2
    flip_z = lambda a: a ^ 8
    turn_z = lambda a: (3 - a // 8) * 8 + a % 8
    other = send(ty, lambda a: a ^ 1)
    xpay = near(lax.ppermute(xown, "gx", around(lax.axis_size("gx"), 1)))
    zpay = near(lax.ppermute(zown, "gz", around(lax.axis_size("gz"), 1)))
    pair = call(pair_kernel, vm(256, LANES), [], [ty, other])
    y_parts = [send(pair, flip_y), send(pair, turn_y), send(pair, lambda a: turn_y(flip_y(a)))]
    below, plane = call(plane_kernel, (vm(256, LANES), vm(256, LANES)), [], [other, pair] + y_parts)
    z_parts = [send(plane, flip_z), send(plane, turn_z), send(plane, lambda a: turn_z(flip_z(a)))]

    big = (TILES, PHOTON, LANES)
    mid = (TILES, KINDS, LANES)
    (ost, g2, pg, cb, made, lost, heat, den, na, yl, yu, zc) = call(
        local_kernel,
        (
            vm(128, 192, dtype=BF16), vm(384, 128, dtype=BF16), vm(144, 512, dtype=BF16),
            vm(320, LANES),
            vm(*mid), vm(*mid), vm(TILES, LANES), vm(TILES, LANES), vm(*big), vm(*big),
            vm(*big), vm(TILES * KINDS, LANES),
        ),
        [illumination],
        [
            n2, temp, opacity_area.T, participant_indices, exothermic_energy[None],
            arrhenius_coefficient[None], arrhenius_barrier[None], emission_loss[None],
        ],
    )
    pe, tiles = call(
        early_kernel, (vm(*big), vm(8, LANES, dtype=jnp.int32)), [illumination, listed],
        [n2, zc, xown, xpay, zown, zpay, ost],
    )
    up, half, ph, cur, curt = call(
        chemistry_kernel,
        (vm(528, LANES), vm(TILES, LANES), vm(*big), vm(MAXD, KINDS, LANES), vm(8, LANES)),
        [],
        [
            tiles, n2, temp, v, ty, below, plane, *z_parts, pe, ost, g2, pg, cb,
            made, lost, heat, den, na, yl, yu,
        ],
    )
    low = near(lax.ppermute(up, "gy", around(size, 1)))
    temp_new, dn, zs = call(
        lower_kernel,
        (vm(TILES, LANES), vm(528, LANES), vm(80, LANES)),
        [],
        [tiles, n2, temp, v, ph, pg, made, lost, heat, den, na, cur, curt, up, half],
    )
    high = near(lax.ppermute(dn, "gy", around(size, -1)))
    hz = near(lax.ppermute(zs, "gz", around(lax.axis_size("gz"), 1)))
    xdn = near(lax.ppermute(dn, "gx", around(lax.axis_size("gx"), 1)))
    xup = near(lax.ppermute(up, "gx", around(lax.axis_size("gx"), 1)))
    acc = call(inner_kernel, vm(*mid), [], [dn, up, v, xdn, xup])
    out = call(
        outer_kernel, hbm(KINDS * TILES, LANES), [],
        [dn, up, acc, v, low, high, zs, hz],
    )
    return out.reshape(KINDS, 4, 4, LANES), temp_new.reshape(4, 4, LANES)


def solution(mesh):
    field = P(None, "gx", "gy", "gz")
    return jax.shard_map(
        shards,
        mesh=mesh,
        in_specs=(field, P("gx", "gy", "gz"), field) + (P(),) * 7 + (P("gx", "gy", "gz", None),),
        out_specs=(field, P("gx", "gy", "gz")),
        check_vma=False,
    )
```
